32 devices in a mesh: groups: 2 (over y), seq: 16 (over z, x, core).
Axes of the slice: x: 2, y: 2, z: 4, core: 2. Of those that a mesh axis runs over, the one named last changes fastest.
Arguments:
- queries: bfloat16 [8192, 4096], P(('groups', 'seq')), parts along dimension 0
- new_keys: bfloat16 [8192, 1024], P(('groups', 'seq')), parts along dimension 0
- new_values: bfloat16 [8192, 1024], P(('groups', 'seq')), parts along dimension 0, may hold values from -6 to 6
- pool_keys: bfloat16 [672, 16, 1024], P(('groups', 'seq')), parts along dimension 0, may hold values from -10 to 10
- pool_values: bfloat16 [672, 16, 1024], P(('groups', 'seq')), parts along dimension 0, may hold values from -6 to 6
- prefix_len: int32 [32], P(('groups', 'seq')), parts along dimension 0, may hold values from 1 to 80
- new_len: int32 [32], P(('groups', 'seq')), parts along dimension 0, may hold values from 128 to 256
- page_holder: int32 [32, 5], P(('groups', 'seq')), parts along dimension 0, may hold values from 0 to 15, as said below
- page_slot: int32 [32, 5], P(('groups', 'seq')), parts along dimension 0, may hold values from 0 to 20, as said below
- new_holder: int32 [32, 16], P(('groups', 'seq')), parts along dimension 0, may hold values from 0 to 15, as said below
- new_slot: int32 [32, 16], P(('groups', 'seq')), parts along dimension 0, may hold values from 0 to 20
Outputs:
- attention_out: bfloat16 [8192, 4096], P(('groups', 'seq')), parts along dimension 0
- pool_keys_out: bfloat16 [672, 16, 1024], P(('groups', 'seq')), parts along dimension 0
- pool_values_out: bfloat16 [672, 16, 1024], P(('groups', 'seq')), parts along dimension 0
The draws below stay inside these ranges and needn't reach their ends.
There are 2 independent parts, one for each index of `groups`. The reference program is written for one: setup_inputs(seed, part) draws one part's arguments, and reference() takes and returns one part's arrays. A program takes and returns all parts, laid end to end along the dimension named above; each array names one. Nothing has to cross between parts.
Inputs may be any that keep to these rules, and one draw needn't show every extreme that they name: `page_holder`: the 5 pages named for one conversation lie on distinct devices. No pool slot is named twice by page_slot and new_slot together, and no slot named by new_slot is named by page_slot. `new_holder`: the 16 pages of one conversation's new turn go to distinct devices.
All inputs are finite; a program needn't handle non-finite values.
Results may differ from the reference program's by a relative error of at most 0.0027.
Values may be sent and summed in bfloat16 or wider, within the bound.
A program may use at most 128 MiB of HBM per device.

```python
import math
import jax
import jax.numpy as jnp
from jax import lax

HEADS = 32
KV_HEADS = 8
HEAD = 128
SPAN = 256
PAGE = 16
KVW = 1024
MAXPRE = 5
NEWP = 16
POOL = 21
TOKENS = 4096
SLOTS = 336
N_SEQ = 16


def attention_draws(key):
    base_key = jax.random.fold_in(key, 11)
    query_key, key_key = jax.random.split(base_key)
    keys_all = 1.7 * jax.random.normal(key_key, (N_SEQ, SPAN, KV_HEADS, HEAD), jnp.float32)
    queries_all = 1.7 * jax.random.normal(query_key, (N_SEQ, SPAN, HEADS, HEAD), jnp.float32)
    return (queries_all.reshape(N_SEQ * SPAN, HEADS * HEAD), keys_all.reshape(N_SEQ * SPAN, KV_HEADS * HEAD))


def draw_queries(key, part):
    return attention_draws(key)[0].astype(jnp.bfloat16)


def draw_new_keys(key, part):
    return attention_draws(key)[1].astype(jnp.bfloat16)


def block_tables(key):
    base_key = jax.random.fold_in(key, 29)
    key_first, key_second, key_third = jax.random.split(base_key, 3)
    order_pre = jax.random.permutation(key_first, N_SEQ).astype(jnp.int32)
    order_new = jax.random.permutation(key_second, N_SEQ).astype(jnp.int32)
    place_pre = jnp.argsort(order_pre).astype(jnp.int32)
    place_new = jnp.argsort(order_new).astype(jnp.int32)
    slot_keys = jax.random.split(key_third, N_SEQ)
    slot_order = jax.vmap(lambda single: jax.random.permutation(single, POOL))(slot_keys).astype(jnp.int32)
    page_ids = jnp.arange(MAXPRE, dtype=jnp.int32)
    fresh_ids = jnp.arange(NEWP, dtype=jnp.int32)
    page_holder = order_pre[(place_pre[:, None] + 1 + page_ids[None, :]) % N_SEQ]
    page_slot = slot_order[page_holder, jnp.broadcast_to(page_ids[None, :], page_holder.shape)]
    new_holder = order_new[(place_new[:, None] + 1 + fresh_ids[None, :]) % N_SEQ]
    new_slot = slot_order[new_holder, jnp.broadcast_to(MAXPRE + fresh_ids[None, :], new_holder.shape)]
    return (page_holder.astype(jnp.int32), page_slot.astype(jnp.int32), new_holder.astype(jnp.int32), new_slot.astype(jnp.int32))


def draw_page_holder(key, part):
    return block_tables(key)[0]


def draw_page_slot(key, part):
    return block_tables(key)[1]


def draw_new_holder(key, part):
    return block_tables(key)[2]


def draw_new_slot(key, part):
    return block_tables(key)[3]


def place_ends(entries, stream_key, low, largest):
    extent = entries.shape
    place = [jax.random.randint(jax.random.fold_in(stream_key, axis), (), 0, extent[axis]) for axis in range(len(extent))]
    entries = entries.at[tuple(place)].set(low)
    longest = extent.index(max(extent))
    place[longest] = (place[longest] + 1) % extent[longest]
    return entries.at[tuple(place)].set(largest)


def level_of(own_key, shape, shards, smallest, largest):
    level = 1.0
    for position, parts in shards:
        steps = jax.random.uniform(jax.random.fold_in(jax.random.fold_in(own_key, 6), position), (parts,), jnp.float32, smallest / len(shards), largest / len(shards))
        level = level * jnp.repeat(jnp.exp(steps), shape[position] // parts).reshape((-1,) + (1,) * (len(shape) - 1 - position))
    return level


def bell_draw(own_key, dims, width, limit, pieces=(), kind=jnp.bfloat16):
    drawn = jax.random.normal(own_key, dims, jnp.float32) * width
    if len(pieces) > 0:
        drawn = level_of(own_key, dims, pieces, -0.22, 0.18) * drawn
    return jnp.clip(drawn, min=-limit, max=limit).astype(kind)


def setup_inputs(seed: int = 0, part: int = 0) -> dict:
    key_list = jax.random.split(jax.random.key(seed), 12)
    part_splits = jax.random.split(jax.random.fold_in(key_list[11], part), 12)
    return {
        "queries": draw_queries(jax.random.fold_in(jax.random.fold_in(key_list[11], part), 71), part),
        "new_keys": draw_new_keys(jax.random.fold_in(jax.random.fold_in(key_list[11], part), 71), part),
        "new_values": bell_draw(part_splits[2], (TOKENS, KVW), 1.0, 6.0, ((0, 16),)),
        "pool_keys": bell_draw(part_splits[3], (SLOTS, PAGE, KVW), 1.7, 10.0, ((0, 16),)),
        "pool_values": bell_draw(part_splits[4], (SLOTS, PAGE, KVW), 1.0, 6.0, ((0, 16),)),
        "prefix_len": place_ends(jax.random.randint(part_splits[5], (N_SEQ,), 1, MAXPRE * PAGE + 1), jax.random.fold_in(part_splits[5], 1), 1, MAXPRE * PAGE).astype(jnp.int32),
        "new_len": place_ends(jax.random.randint(part_splits[6], (N_SEQ,), SPAN // 2, SPAN + 1), jax.random.fold_in(part_splits[6], 1), SPAN // 2, SPAN).astype(jnp.int32),
        "page_holder": draw_page_holder(jax.random.fold_in(jax.random.fold_in(key_list[11], part), 71), part),
        "page_slot": draw_page_slot(jax.random.fold_in(jax.random.fold_in(key_list[11], part), 71), part),
        "new_holder": draw_new_holder(jax.random.fold_in(jax.random.fold_in(key_list[11], part), 71), part),
        "new_slot": draw_new_slot(jax.random.fold_in(jax.random.fold_in(key_list[11], part), 71), part),
    }


def attend(query_rows, prefix_keys, prefix_values, fresh_keys, fresh_values, prefix_tokens, fresh_tokens):
    group_size = HEADS // KV_HEADS
    scaling = 1.0 / math.sqrt(HEAD)
    key_rows = prefix_keys.shape[0]
    prefix_live = jnp.arange(key_rows, dtype=jnp.int32) < prefix_tokens
    token_pos = jnp.arange(SPAN, dtype=jnp.int32)
    fresh_live = (token_pos[None, :] <= token_pos[:, None]) & (token_pos[None, :] < fresh_tokens)
    blocks = []
    for head_group in range(KV_HEADS):
        first_col = head_group * group_size * HEAD
        query_block = query_rows[:, first_col:first_col + group_size * HEAD].reshape(SPAN, group_size, HEAD).astype(jnp.float32)
        key_first = head_group * HEAD
        prefix_key_slice = prefix_keys[:, key_first:key_first + HEAD].astype(jnp.float32)
        prefix_value_slice = prefix_values[:, key_first:key_first + HEAD].astype(jnp.float32)
        fresh_key_slice = fresh_keys[:, key_first:key_first + HEAD].astype(jnp.float32)
        fresh_value_slice = fresh_values[:, key_first:key_first + HEAD].astype(jnp.float32)
        prefix_scores = jnp.einsum('tgd,kd->tgk', query_block, prefix_key_slice, precision=lax.Precision.HIGHEST) * scaling
        fresh_scores = jnp.einsum('tgd,kd->tgk', query_block, fresh_key_slice, precision=lax.Precision.HIGHEST) * scaling
        prefix_scores = jnp.where(prefix_live[None, None, :], prefix_scores, -jnp.inf)
        fresh_scores = jnp.where(fresh_live[:, None, :], fresh_scores, -jnp.inf)
        row_top = jnp.maximum(lax.optimization_barrier(jnp.max(prefix_scores, axis=-1)), lax.optimization_barrier(jnp.max(fresh_scores, axis=-1)))[..., None]
        prefix_weights = jnp.exp(prefix_scores - row_top)
        fresh_weights = jnp.exp(fresh_scores - row_top)
        weight_sum = lax.optimization_barrier(jnp.sum(prefix_weights, axis=-1)) + lax.optimization_barrier(jnp.sum(fresh_weights, axis=-1))
        prefix_round = lax.optimization_barrier(prefix_weights.astype(jnp.bfloat16)).astype(jnp.float32)
        fresh_round = lax.optimization_barrier(fresh_weights.astype(jnp.bfloat16)).astype(jnp.float32)
        weighted = jnp.einsum('tgk,kd->tgd', prefix_round, prefix_value_slice, precision=lax.Precision.HIGHEST)
        weighted = weighted + jnp.einsum('tgk,kd->tgd', fresh_round, fresh_value_slice, precision=lax.Precision.HIGHEST)
        blocks.append((weighted / weight_sum[..., None]).reshape(SPAN, group_size * HEAD))
    joined = jnp.concatenate(blocks, axis=1)
    row_live = (token_pos < fresh_tokens)[:, None]
    return jnp.where(row_live, joined, 0.0).astype(jnp.bfloat16)

def reference(queries, new_keys, new_values, pool_keys, pool_values, prefix_len, new_len, page_holder, page_slot, new_holder, new_slot):
    kv_width = KV_HEADS * HEAD

    def conversation(device):
        page_rows = (page_holder[device] * POOL + page_slot[device]).astype(jnp.int32)
        prefix_keys = jnp.take(pool_keys, page_rows, axis=0).reshape(MAXPRE * PAGE, kv_width)
        prefix_values = jnp.take(pool_values, page_rows, axis=0).reshape(MAXPRE * PAGE, kv_width)
        row_start = (device * SPAN).astype(jnp.int32)
        query_rows = lax.dynamic_slice_in_dim(queries, row_start, SPAN, 0)
        fresh_keys = lax.dynamic_slice_in_dim(new_keys, row_start, SPAN, 0)
        fresh_values = lax.dynamic_slice_in_dim(new_values, row_start, SPAN, 0)
        return attend(query_rows, prefix_keys, prefix_values, fresh_keys, fresh_values, prefix_len[device], new_len[device])
    outputs = lax.map(conversation, jnp.arange(N_SEQ, dtype=jnp.int32))
    attention_out = outputs.reshape(N_SEQ * SPAN, HEADS * HEAD)
    token_pos = jnp.arange(N_SEQ * SPAN, dtype=jnp.int32) % SPAN
    row_keep = (token_pos < jnp.repeat(new_len, SPAN))[:, None]
    kept_keys = jnp.where(row_keep, new_keys, 0).reshape(N_SEQ * NEWP, PAGE, kv_width)
    kept_values = jnp.where(row_keep, new_values, 0).reshape(N_SEQ * NEWP, PAGE, kv_width)
    targets = (new_holder * POOL + new_slot).reshape(-1).astype(jnp.int32)
    pool_keys_out = pool_keys.at[targets].set(kept_keys)
    pool_values_out = pool_values.at[targets].set(kept_values)
    return (attention_out, pool_keys_out, pool_values_out)
```

```python
import functools
import math

import jax
import jax.numpy as jnp
from jax import lax
from jax.experimental import pallas as pl
from jax.experimental.pallas import tpu as pltpu
from jax.sharding import PartitionSpec as P

HEADS = 32
KV_HEADS = 8
HEAD = 128
ROWS = 128
SLOT_LANE = 64
EARLY = 5
FIRST = 1
MESH = pl.DeviceIdType.MESH


def crosses_once(n, new_pages):
    return n == new_pages and n % 4 == 0


def kernel(
    n,
    new_pages,
    prefix_pages,
    prefix_len,
    new_len,
    page_holder,
    page_slot,
    new_holder,
    new_slot,
    q_hbm,
    k_hbm,
    v_hbm,
    pk_hbm,
    pv_hbm,
    out,
    recv_new,
    pool,
    source,
    q,
    kv,
    prefix,
    send_new,
    meta,
    recv_meta,
    tables,
    in_sem,
    table_sem,
    meta_send_sem,
    meta_recv_sem,
    new_send_sem,
    new_recv_sem,
    *exchange,
):
    me = lax.axis_index("seq")
    mine = lax.axis_index("groups")
    halves = crosses_once(n, new_pages)
    span = q.shape[0]
    page_rows = pool.shape[2]
    slots = pool.shape[1]
    group = HEADS // KV_HEADS

    loads = [
        pltpu.make_async_copy(k_hbm, kv.at[0], in_sem.at[0]),
        pltpu.make_async_copy(v_hbm, kv.at[1], in_sem.at[1]),
        pltpu.make_async_copy(pk_hbm, pool.at[0], in_sem.at[2]),
        pltpu.make_async_copy(pv_hbm, pool.at[1], in_sem.at[3]),
        pltpu.make_async_copy(q_hbm, q, in_sem.at[4]),
    ]
    for load in loads:
        load.start()

    def peer(step):
        return lax.rem(me + step, n)

    barrier = pltpu.get_barrier_semaphore()

    def greet(step, carry):
        pl.semaphore_signal(barrier, inc=1, device_id=(mine, peer(step)), device_id_type=MESH)
        return carry

    lax.fori_loop(1, n, greet, 0)

    lanes = lax.broadcasted_iota(jnp.int32, meta.shape, 1)
    row = jnp.full(meta.shape, -1, jnp.int32)
    for i in range(new_pages):
        row = jnp.where(lanes == i, new_holder[0, i], row)
        row = jnp.where(lanes == SLOT_LANE + i, new_slot[0, i], row)
    for j in range(prefix_pages):
        row = jnp.where(lanes == new_pages + j, page_holder[0, j], row)
        row = jnp.where(lanes == SLOT_LANE + new_pages + j, page_slot[0, j], row)
    meta[...] = row
    recv_meta[me] = row

    prefix[...] = jnp.zeros_like(prefix)
    live = new_len[0]
    loads[0].wait()
    loads[1].wait()
    page_pos = lax.broadcasted_iota(jnp.int32, (page_rows, kv.shape[3]), 0)

    def fill_new(target, carry):
        page = jnp.int32(0)
        for i in range(new_pages):
            page = jnp.where(new_holder[0, i] == target, i, page)
        keep = page_pos < live - page * page_rows
        for side in range(2):
            rows = kv[side, page]
            send_new[target, side] = jnp.where(keep, rows, jnp.zeros_like(rows))
        return carry

    lax.fori_loop(0, n, fill_new, 0)
    recv_new[me] = send_new[me]

    def remote(sent, received, send_sem, recv_sem, target):
        return pltpu.make_async_remote_copy(
            src_ref=sent,
            dst_ref=received,
            send_sem=send_sem,
            recv_sem=recv_sem,
            device_id=(mine, target),
            device_id_type=MESH,
        )

    def landed(buffer, sem):
        return pltpu.make_async_copy(buffer, buffer, sem)

    def meta_copy(step):
        return remote(
            meta, recv_meta.at[me], meta_send_sem.at[step], meta_recv_sem.at[me], peer(step)
        )

    def new_to(target):
        return remote(
            send_new.at[target],
            recv_new.at[me],
            new_send_sem.at[target],
            new_recv_sem.at[me],
            target,
        )

    def arrival(step, buffer, sem):
        at = peer(step)
        return landed(buffer.at[at], sem.at[at])

    pl.semaphore_wait(barrier, n - 1)

    def each(first, last, act):
        def body(step, carry):
            act(step)
            return carry

        lax.fori_loop(first, last, body, 0)

    each(1, n, lambda step: meta_copy(step).start())

    def wanted(conversation, holder):
        slot = jnp.int32(-1)
        for j in range(prefix_pages):
            slot = jnp.where(
                tables[conversation, 0, new_pages + j] == holder,
                tables[conversation, 0, SLOT_LANE + new_pages + j],
                slot,
            )
        return slot

    def read_tables():
        each(1, n, lambda step: arrival(step, recv_meta, meta_recv_sem).wait())
        table_copy = pltpu.make_async_copy(recv_meta, tables, table_sem)
        table_copy.start()
        table_copy.wait()

    def index_incoming():
        def clear(slot):
            source[slot] = -1

        each(0, slots, clear)

        def incoming(device):
            landing = jnp.int32(-1)
            for i in range(new_pages):
                landing = jnp.where(
                    tables[device, 0, i] == me, tables[device, 0, SLOT_LANE + i], landing
                )

            for slot in range(slots):
                source[slot] = jnp.where(landing == slot, device, source[slot])

        each(0, n, incoming)

    if halves:
        (
            mirror_k,
            mirror_v,
            mirrored_k,
            mirrored_v,
            send_own,
            recv_own,
            relay_k,
            relay_v,
            recv_k,
            recv_v,
            ranks,
            mirror_send_sem,
            mirror_recv_sem,
            own_send_sem,
            own_recv_sem,
            relay_send_sem,
            relay_recv_sem,
        ) = exchange
        half, plane = n // 2, n // 4
        layer, place = me // plane, lax.rem(me, plane)
        mine_half = me // half
        base, other = mine_half * half, (1 - mine_half) * half
        inner = (layer == 1) | (layer == 2)
        here = me - base
        kept = mirror_k.shape[0]

        def in_layer(which, i):
            return which * plane + lax.rem(place + i, plane)

        beside = base // plane + 1 - lax.rem(layer, 2)
        near = 2 - mine_half
        far = 3 - 3 * mine_half

        def send_layer(which, first, last):
            each(first, last, lambda i: new_to(in_layer(which, i)).start())

        send_layer(far, 0, FIRST)
        send_layer(layer, 1, plane)

        mirror_at = half - plane * mine_half + place
        origin = lax.rem(layer, 2)

        def mirror_copy(which, sent, received):
            return remote(
                sent,
                received.at[origin],
                mirror_send_sem.at[which],
                mirror_recv_sem.at[origin, which],
                mirror_at,
            )

        def half_peer(i):
            return lax.rem(here + i, half)

        def own_copy(i):
            to = half_peer(i)
            return remote(
                send_own.at[to],
                recv_own.at[here],
                own_send_sem.at[to],
                own_recv_sem.at[here],
                base + to,
            )

        def relay_copy(i, which):
            to = half_peer(i)
            sent, received = ((relay_k, recv_k), (relay_v, recv_v))[which]
            return remote(
                sent.at[to],
                received.at[place],
                relay_send_sem.at[to, which],
                relay_recv_sem.at[place, which],
                base + to,
            )

        loads[2].wait()
        loads[3].wait()
        read_tables()

        def pick(i, carry):
            count, picks = carry
            slot = wanted(other + i, me)
            found = slot >= 0
            picks = tuple(
                jnp.where(found & (count == k), slot, p) for k, p in enumerate(picks)
            )
            return count + jnp.where(found, 1, 0), picks

        picks = lax.fori_loop(
            0, half, pick, (jnp.int32(0), (jnp.int32(0),) * kept)
        )[1]
        for k in range(kept):
            mirror_k[k] = pool[0, picks[k]]
        for k in range(kept):
            mirror_v[k] = pool[1, picks[k]]
        mirror_copy(0, mirror_k, mirrored_k).start()
        mirror_copy(1, mirror_v, mirrored_v).start()

        def fill_own(i):
            to = half_peer(i)
            slot = jnp.maximum(wanted(base + to, me), 0)
            for side in range(2):
                send_own[to, side] = pool[side, slot]

        fill_own(1)

        def own_step(i):
            fill_own(i)
            own_copy(i - 1).start()

        each(2, half, own_step)
        fill_own(0)
        own_copy(half - 1).start()
        recv_own[here] = send_own[here]

        send_layer(beside, 0, plane)
        send_layer(near, 0, plane)

        @pl.when(inner)
        def _():
            for o in range(2):
                def rank(i, count):
                    ranks[i * 2 + o] = jnp.minimum(count, kept - 1)
                    found = wanted(base + i, other + o * plane + place) >= 0
                    return count + jnp.where(found, 1, 0)

                lax.fori_loop(0, half, rank, jnp.int32(0))

            for which in range(2):
                sent, got = ((relay_k, mirrored_k), (relay_v, mirrored_v))[which]
                received = (recv_k, recv_v)[which]
                for o in range(2):
                    landed(got.at[o], mirror_recv_sem.at[o, which]).wait()

                def fill_relay(i):
                    to = half_peer(i)
                    for o in range(2):
                        sent[to, o] = got[o, ranks[to * 2 + o]]

                fill_relay(1)

                def relay_step(i):
                    fill_relay(i)
                    relay_copy(i - 1, which).start()

                each(2, half, relay_step)
                fill_relay(0)
                relay_copy(half - 1, which).start()
                received[place] = sent[here]
            send_layer(far, FIRST, plane)

        index_incoming()
        loads[4].wait()

        each(1, half, lambda i: landed(
            recv_own.at[half_peer(i)], own_recv_sem.at[half_peer(i)]
        ).wait())
        for which in range(2):
            received = (recv_k, recv_v)[which]

            def relayed(i):
                @pl.when(jnp.logical_not(inner & (i == place)))
                def _():
                    landed(received.at[i], relay_recv_sem.at[i, which]).wait()

            each(0, plane, relayed)

        @pl.when(jnp.logical_not(inner))
        def _():
            send_layer(far, FIRST, plane)

        for j in range(prefix_pages):
            holder = page_holder[0, j]
            close = holder // half == mine_half
            for side in range(2):
                own = recv_own[lax.rem(holder, half), side]
                through = (recv_k, recv_v)[side][
                    lax.rem(holder, plane), lax.rem(holder // plane, 2)
                ]
                prefix[side, j * page_rows : (j + 1) * page_rows, :] = jnp.where(
                    close, own, through
                )

        def sent_pages():
            mirror_copy(0, mirror_k, mirrored_k).wait_send()
            mirror_copy(1, mirror_v, mirrored_v).wait_send()
            each(1, half, lambda i: own_copy(i).wait_send())

            @pl.when(inner)
            def _():
                for which in range(2):
                    each(1, half, lambda i: relay_copy(i, which).wait_send())

    else:
        send_pre, recv_pre, pre_send_sem, pre_recv_sem = exchange

        def pre_copy(step):
            return remote(
                send_pre.at[peer(step)],
                recv_pre.at[me],
                pre_send_sem.at[step],
                pre_recv_sem.at[me],
                peer(step),
            )

        early = min(EARLY, n - 1) + 1
        each(1, early, lambda step: new_to(peer(step)).start())
        loads[2].wait()
        loads[3].wait()
        read_tables()

        def fill_pre(target):
            slot = jnp.maximum(wanted(target, me), 0)
            for side in range(2):
                send_pre[target, side] = pool[side, slot]

        fill_pre(peer(1))

        def pipelined(step):
            fill_pre(peer(step))
            pre_copy(step - 1).start()

        each(2, n, pipelined)
        fill_pre(me)
        pre_copy(n - 1).start()
        recv_pre[me] = send_pre[me]
        each(early, n, lambda step: new_to(peer(step)).start())
        index_incoming()
        loads[4].wait()

        each(1, n, lambda step: arrival(step, recv_pre, pre_recv_sem).wait())
        for j in range(prefix_pages):
            for side in range(2):
                prefix[side, j * page_rows : (j + 1) * page_rows, :] = recv_pre[
                    page_holder[0, j], side
                ]

        def sent_pages():
            each(1, n, lambda step: pre_copy(step).wait_send())

    factor = math.log2(math.e) / math.sqrt(HEAD)
    nt = (((1,), (1,)), ((), ()))
    row_pos = lax.rem(lax.broadcasted_iota(jnp.int32, (group * ROWS, ROWS), 0), ROWS)
    col_pos = lax.broadcasted_iota(jnp.int32, (group * ROWS, ROWS), 1)
    prefix_pos = lax.broadcasted_iota(jnp.int32, (group * ROWS, prefix.shape[1]), 1)
    prefix_tokens = prefix_len[0]

    def head_cols(g, h):
        return pl.ds(pl.multiple_of((g * group + h) * HEAD, HEAD), HEAD)

    def attend(g):
        kv_cols = pl.ds(pl.multiple_of(g * HEAD, HEAD), HEAD)
        for block in range(span // ROWS):
            rows = slice(block * ROWS, (block + 1) * ROWS)
            keys = (block + 1) * ROWS
            query = jnp.concatenate(
                [q[rows, head_cols(g, h)] for h in range(group)], axis=0
            )
            old = lax.dot_general(
                query, prefix[0, :, kv_cols], nt, preferred_element_type=jnp.float32
            )
            fresh = lax.dot_general(
                query,
                kv[0, : keys // page_rows, :, kv_cols].reshape(keys, HEAD),
                nt,
                preferred_element_type=jnp.float32,
            )
            old = jnp.where(prefix_pos < prefix_tokens, old, -jnp.inf)
            last = jnp.where(col_pos <= row_pos, fresh[:, block * ROWS :], -jnp.inf)
            parts = [fresh[:, i * ROWS : (i + 1) * ROWS] for i in range(block)] + [last]
            top = old
            for part in parts:
                top = jnp.maximum(top, part)
            top = jnp.max(top, axis=1, keepdims=True)
            old = jnp.exp2((old - top) * factor)
            parts = [jnp.exp2((part - top) * factor) for part in parts]
            total = old
            for part in parts:
                total = total + part
            total = jnp.sum(total, axis=1, keepdims=True)
            weighted = jnp.dot(
                old.astype(jnp.bfloat16),
                prefix[1, :, kv_cols],
                preferred_element_type=jnp.float32,
            )
            weighted = weighted + jnp.dot(
                jnp.concatenate(parts, axis=1).astype(jnp.bfloat16),
                kv[1, : keys // page_rows, :, kv_cols].reshape(keys, HEAD),
                preferred_element_type=jnp.float32,
            )
            result = weighted * (1.0 / total)
            result = jnp.where(row_pos + block * ROWS < live, result, 0.0).astype(jnp.bfloat16)
            for h in range(group):
                out[rows, head_cols(g, h)] = result[h * ROWS : (h + 1) * ROWS]

    each(0, KV_HEADS, attend)

    each(1, n, lambda step: arrival(step, recv_new, new_recv_sem).wait())
    each(1, n, lambda step: meta_copy(step).wait_send())
    each(1, n, lambda step: new_to(peer(step)).wait_send())
    sent_pages()


def finish(source, out, recv_new, pool, o_hbm, pko_hbm, pvo_hbm, pool_out, sem):
    slots = pool.shape[1]
    whole = pltpu.make_async_copy(out, o_hbm, sem.at[0])
    whole.start()

    def place(slot, carry):
        device = source[slot]
        found = device >= 0
        for side in range(2):
            pool_out[side, slot] = jnp.where(
                found, recv_new[jnp.maximum(device, 0), side], pool[side, slot]
            )
        return carry

    lax.fori_loop(0, slots, place, 0)
    stores = [
        pltpu.make_async_copy(pool_out.at[0], pko_hbm, sem.at[1]),
        pltpu.make_async_copy(pool_out.at[1], pvo_hbm, sem.at[2]),
    ]
    for store in stores:
        store.start()
    for store in stores:
        store.wait()
    whole.wait()


def shards(
    queries,
    new_keys,
    new_values,
    pool_keys,
    pool_values,
    prefix_len,
    new_len,
    page_holder,
    page_slot,
    new_holder,
    new_slot,
):
    n = lax.axis_size("seq")
    slots, page_rows, width = pool_keys.shape
    span = queries.shape[0]
    new_pages = new_holder.shape[1]
    prefix_pages = page_holder.shape[1]
    padded = -(-prefix_pages * page_rows // ROWS) * ROWS
    kind = queries.dtype
    smem = pl.BlockSpec(memory_space=pltpu.SMEM)
    anywhere = pl.BlockSpec(memory_space=pl.ANY)
    peers = pltpu.SemaphoreType.DMA((n,))

    def pages(*count):
        return pltpu.VMEM((*count, page_rows, width), kind)

    if crosses_once(n, new_pages):
        half, plane, left = n // 2, n // 4, slots - new_pages
        exchange = [
            pages(left),
            pages(left),
            pages(2, left),
            pages(2, left),
            pages(half, 2),
            pages(half, 2),
            pages(half, 2),
            pages(half, 2),
            pages(plane, 2),
            pages(plane, 2),
            pltpu.SMEM((n,), jnp.int32),
            pltpu.SemaphoreType.DMA((2,)),
            pltpu.SemaphoreType.DMA((2, 2)),
            pltpu.SemaphoreType.DMA((half,)),
            pltpu.SemaphoreType.DMA((half,)),
            pltpu.SemaphoreType.DMA((half, 2)),
            pltpu.SemaphoreType.DMA((plane, 2)),
        ]
    else:
        exchange = [pages(n, 2), pages(n, 2), peers, peers]
    held = pl.BlockSpec(memory_space=pltpu.VMEM)
    page_bytes = 2 * page_rows * width * kind.itemsize
    kept = queries.size * kind.itemsize + (n + slots) * page_bytes
    grant = 67043328 - kept - 256 * 1024
    results = (
        jax.ShapeDtypeStruct(queries.shape, kind),
        jax.ShapeDtypeStruct(pool_keys.shape, kind),
        jax.ShapeDtypeStruct(pool_values.shape, kind),
    )
    out, recv_new, pool, source = pl.pallas_call(
        functools.partial(kernel, n, new_pages, prefix_pages),
        out_shape=(
            pltpu.VMEM(queries.shape, kind),
            pltpu.VMEM((n, 2, page_rows, width), kind),
            pltpu.VMEM((2, slots, page_rows, width), kind),
            jax.ShapeDtypeStruct((slots,), jnp.int32),
        ),
        in_specs=[smem] * 6 + [anywhere] * 5,
        out_specs=(held, held, held, smem),
        scratch_shapes=[
            pltpu.VMEM(queries.shape, kind),
            pltpu.VMEM((2, span // page_rows, page_rows, width), kind),
            pltpu.VMEM((2, padded, width), kind),
            pages(n, 2),
            pltpu.VMEM((1, 128), jnp.int32),
            pltpu.VMEM((n, 1, 128), jnp.int32),
            pltpu.SMEM((n, 1, 128), jnp.int32),
            pltpu.SemaphoreType.DMA((5,)),
            pltpu.SemaphoreType.DMA,
            peers,
            peers,
            peers,
            peers,
            *exchange,
        ],
        compiler_params=pltpu.CompilerParams(
            collective_id=0, has_side_effects=True, vmem_limit_bytes=grant
        ),
    )(
        prefix_len,
        new_len,
        page_holder,
        page_slot,
        new_holder,
        new_slot,
        queries,
        new_keys.reshape(span // page_rows, page_rows, width),
        new_values.reshape(span // page_rows, page_rows, width),
        pool_keys,
        pool_values,
    )
    return pl.pallas_call(
        finish,
        out_shape=results,
        in_specs=[smem, held, held, held],
        out_specs=(anywhere,) * 3,
        scratch_shapes=[
            pltpu.VMEM((2, slots, page_rows, width), kind),
            pltpu.SemaphoreType.DMA((3,)),
        ],
        compiler_params=pltpu.CompilerParams(
            vmem_limit_bytes=slots * page_bytes + 4 * 1024 * 1024
        ),
    )(source, out, recv_new, pool)


def solution(mesh):
    rows = P(("groups", "seq"), None)
    pages = P(("groups", "seq"), None, None)
    each = P(("groups", "seq"))
    return jax.shard_map(
        shards,
        mesh=mesh,
        in_specs=(rows, rows, rows, pages, pages, each, each, rows, rows, rows, rows),
        out_specs=(rows, pages, pages),
        check_vma=False,
    )
```

```python
import functools
import math

import jax
import jax.numpy as jnp
from jax import lax
from jax.experimental import pallas as pl
from jax.experimental.pallas import tpu as pltpu
from jax.sharding import PartitionSpec as P

HEADS = 32
KV_HEADS = 8
HEAD = 128
ROWS = 128
SLOT_LANE = 64
EARLY = 5
FIRST = 2
MESH = pl.DeviceIdType.MESH


def crosses_once(n, new_pages):
    return n == new_pages and n % 4 == 0


def kernel(
    n,
    new_pages,
    prefix_pages,
    prefix_len_hbm,
    new_len_hbm,
    page_holder_hbm,
    page_slot_hbm,
    new_holder_hbm,
    new_slot_hbm,
    q_hbm,
    k_hbm,
    v_hbm,
    pk_hbm,
    pv_hbm,
    out,
    pool_out,
    recv_new,
    pool,
    source,
    prefix_len,
    new_len,
    page_holder,
    page_slot,
    new_holder,
    new_slot,
    q,
    kv,
    prefix,
    send_new,
    meta,
    recv_meta,
    tables,
    in_sem,
    own_sem,
    table_sem,
    meta_send_sem,
    meta_recv_sem,
    new_send_sem,
    new_recv_sem,
    *exchange,
):
    me = lax.axis_index("seq")
    mine = lax.axis_index("groups")
    halves = crosses_once(n, new_pages)
    span = q.shape[0]
    page_rows = pool.shape[2]
    slots = pool.shape[1]
    group = HEADS // KV_HEADS

    def peer(step):
        return lax.rem(me + step, n)

    barrier = pltpu.get_barrier_semaphore()

    def greet(step, carry):
        pl.semaphore_signal(barrier, inc=1, device_id=(mine, peer(step)), device_id_type=MESH)
        return carry

    lax.fori_loop(1, n, greet, 0)

    given = [
        pltpu.make_async_copy(there, here, own_sem.at[i])
        for i, (there, here) in enumerate(
            (
                (new_holder_hbm, new_holder),
                (new_slot_hbm, new_slot),
                (page_holder_hbm, page_holder),
                (page_slot_hbm, page_slot),
                (new_len_hbm, new_len),
                (prefix_len_hbm, prefix_len),
            )
        )
    ]
    for copy in given:
        copy.start()
    loads = [
        pltpu.make_async_copy(k_hbm, kv.at[0], in_sem.at[0]),
        pltpu.make_async_copy(v_hbm, kv.at[1], in_sem.at[1]),
        pltpu.make_async_copy(pk_hbm, pool.at[0], in_sem.at[2]),
        pltpu.make_async_copy(pv_hbm, pool.at[1], in_sem.at[3]),
        pltpu.make_async_copy(q_hbm, q, in_sem.at[4]),
    ]
    for load in loads:
        load.start()

    for copy in given:
        copy.wait()

    lanes = lax.broadcasted_iota(jnp.int32, meta.shape, 1)
    row = jnp.full(meta.shape, -1, jnp.int32)
    for i in range(new_pages):
        row = jnp.where(lanes == i, new_holder[0, i], row)
        row = jnp.where(lanes == SLOT_LANE + i, new_slot[0, i], row)
    for j in range(prefix_pages):
        row = jnp.where(lanes == new_pages + j, page_holder[0, j], row)
        row = jnp.where(lanes == SLOT_LANE + new_pages + j, page_slot[0, j], row)
    meta[...] = row
    recv_meta[me] = row

    live = new_len[0]
    page_pos = lax.broadcasted_iota(jnp.int32, (page_rows, kv.shape[3]), 0)

    def fill_new(target):
        page = jnp.int32(0)
        for i in range(new_pages):
            page = jnp.where(new_holder[0, i] == target, i, page)
        keep = page_pos < live - page * page_rows
        for side in range(2):
            rows = kv[side, page]
            send_new[target, side] = jnp.where(keep, rows, jnp.zeros_like(rows))

    def remote(sent, received, send_sem, recv_sem, target):
        return pltpu.make_async_remote_copy(
            src_ref=sent,
            dst_ref=received,
            send_sem=send_sem,
            recv_sem=recv_sem,
            device_id=(mine, target),
            device_id_type=MESH,
        )

    def landed(buffer, sem):
        return pltpu.make_async_copy(buffer, buffer, sem)

    def meta_copy(step):
        return remote(
            meta, recv_meta.at[me], meta_send_sem.at[step], meta_recv_sem.at[me], peer(step)
        )

    def new_to(target):
        return remote(
            send_new.at[target],
            recv_new.at[me],
            new_send_sem.at[target],
            new_recv_sem.at[me],
            target,
        )

    def arrival(step, buffer, sem):
        at = peer(step)
        return landed(buffer.at[at], sem.at[at])

    pl.semaphore_wait(barrier, n - 1)

    def each(first, last, act):
        def body(step, carry):
            act(step)
            return carry

        lax.fori_loop(first, last, body, 0)

    each(1, n, lambda step: meta_copy(step).start())
    loads[0].wait()
    loads[1].wait()

    def wanted(conversation, holder):
        slot = jnp.int32(-1)
        for j in range(prefix_pages):
            slot = jnp.where(
                tables[conversation, 0, new_pages + j] == holder,
                tables[conversation, 0, SLOT_LANE + new_pages + j],
                slot,
            )
        return slot

    def read_tables():
        each(1, n, lambda step: arrival(step, recv_meta, meta_recv_sem).wait())
        table_copy = pltpu.make_async_copy(recv_meta, tables, table_sem)
        table_copy.start()
        table_copy.wait()

    def index_incoming():
        def clear(slot):
            source[slot] = -1

        each(0, slots, clear)

        def incoming(device):
            landing = jnp.int32(-1)
            for i in range(new_pages):
                landing = jnp.where(
                    tables[device, 0, i] == me, tables[device, 0, SLOT_LANE + i], landing
                )

            for slot in range(slots):
                source[slot] = jnp.where(landing == slot, device, source[slot])

        each(0, n, incoming)

    if halves:
        (
            mirror_k,
            mirror_v,
            mirrored_k,
            mirrored_v,
            send_own,
            recv_own,
            relay_k,
            relay_v,
            recv_k,
            recv_v,
            ranks,
            mirror_send_sem,
            mirror_recv_sem,
            own_send_sem,
            own_recv_sem,
            relay_send_sem,
            relay_recv_sem,
        ) = exchange
        half, plane = n // 2, n // 4
        layer, place = me // plane, lax.rem(me, plane)
        mine_half = me // half
        base, other = mine_half * half, (1 - mine_half) * half
        inner = (layer == 1) | (layer == 2)
        here = me - base
        kept = mirror_k.shape[0]

        def in_layer(which, i):
            return which * plane + lax.rem(place + i, plane)

        beside = base // plane + 1 - lax.rem(layer, 2)
        near = 2 - mine_half
        far = 3 - 3 * mine_half

        def send_layer(which, first, last):
            each(first, last, lambda i: new_to(in_layer(which, i)).start())

        def fill_layer(which, first, last):
            each(first, last, lambda i: fill_new(in_layer(which, i)))

        fill_layer(far, 0, FIRST)
        fill_layer(layer, 1, plane)
        send_layer(far, 0, FIRST)
        fill_layer(layer, 0, 1)
        send_layer(layer, 1, plane)
        recv_new[me] = send_new[me]
        fill_layer(beside, 0, plane)
        fill_layer(near, 0, plane)
        fill_layer(far, FIRST, plane)
        prefix[...] = jnp.zeros_like(prefix)

        mirror_at = half - plane * mine_half + place
        origin = lax.rem(layer, 2)

        def mirror_copy(which, sent, received):
            return remote(
                sent,
                received.at[origin],
                mirror_send_sem.at[which],
                mirror_recv_sem.at[origin, which],
                mirror_at,
            )

        def half_peer(i):
            return lax.rem(here + i, half)

        def own_copy(i):
            to = half_peer(i)
            return remote(
                send_own.at[to],
                recv_own.at[here],
                own_send_sem.at[to],
                own_recv_sem.at[here],
                base + to,
            )

        def relay_copy(i, which):
            to = half_peer(i)
            sent, received = ((relay_k, recv_k), (relay_v, recv_v))[which]
            return remote(
                sent.at[to],
                received.at[place],
                relay_send_sem.at[to, which],
                relay_recv_sem.at[place, which],
                base + to,
            )

        loads[2].wait()
        loads[3].wait()
        read_tables()

        def pick(i, carry):
            count, picks = carry
            slot = wanted(other + i, me)
            found = slot >= 0
            picks = tuple(
                jnp.where(found & (count == k), slot, p) for k, p in enumerate(picks)
            )
            return count + jnp.where(found, 1, 0), picks

        picks = lax.fori_loop(
            0, half, pick, (jnp.int32(0), (jnp.int32(0),) * kept)
        )[1]
        for k in range(kept):
            mirror_k[k] = pool[0, picks[k]]
        for k in range(kept):
            mirror_v[k] = pool[1, picks[k]]
        mirror_copy(0, mirror_k, mirrored_k).start()
        mirror_copy(1, mirror_v, mirrored_v).start()

        def fill_own(i):
            to = half_peer(i)
            slot = jnp.maximum(wanted(base + to, me), 0)
            for side in range(2):
                send_own[to, side] = pool[side, slot]

        fill_own(1)

        def own_step(i):
            fill_own(i)
            own_copy(i - 1).start()

        each(2, half, own_step)
        fill_own(0)
        own_copy(half - 1).start()
        recv_own[here] = send_own[here]

        send_layer(beside, 0, plane)
        send_layer(near, 0, plane)

        @pl.when(inner)
        def _():
            for o in range(2):
                def rank(i, count):
                    ranks[i * 2 + o] = jnp.minimum(count, kept - 1)
                    found = wanted(base + i, other + o * plane + place) >= 0
                    return count + jnp.where(found, 1, 0)

                lax.fori_loop(0, half, rank, jnp.int32(0))

            for which in range(2):
                sent, got = ((relay_k, mirrored_k), (relay_v, mirrored_v))[which]
                received = (recv_k, recv_v)[which]
                for o in range(2):
                    landed(got.at[o], mirror_recv_sem.at[o, which]).wait()

                def fill_relay(i):
                    to = half_peer(i)
                    for o in range(2):
                        sent[to, o] = got[o, ranks[to * 2 + o]]

                fill_relay(1)

                def relay_step(i):
                    fill_relay(i)
                    relay_copy(i - 1, which).start()

                each(2, half, relay_step)
                fill_relay(0)
                relay_copy(half - 1, which).start()
                received[place] = sent[here]
            send_layer(far, FIRST, plane)

        index_incoming()
        loads[4].wait()

        each(1, half, lambda i: landed(
            recv_own.at[half_peer(i)], own_recv_sem.at[half_peer(i)]
        ).wait())
        for which in range(2):
            received = (recv_k, recv_v)[which]

            def relayed(i):
                @pl.when(jnp.logical_not(inner & (i == place)))
                def _():
                    landed(received.at[i], relay_recv_sem.at[i, which]).wait()

            each(0, plane, relayed)

        @pl.when(jnp.logical_not(inner))
        def _():
            send_layer(far, FIRST, plane)

        for j in range(prefix_pages):
            holder = page_holder[0, j]
            close = holder // half == mine_half
            for side in range(2):
                own = recv_own[lax.rem(holder, half), side]
                through = (recv_k, recv_v)[side][
                    lax.rem(holder, plane), lax.rem(holder // plane, 2)
                ]
                prefix[side, j * page_rows : (j + 1) * page_rows, :] = jnp.where(
                    close, own, through
                )

        def sent_pages():
            mirror_copy(0, mirror_k, mirrored_k).wait_send()
            mirror_copy(1, mirror_v, mirrored_v).wait_send()
            each(1, half, lambda i: own_copy(i).wait_send())

            @pl.when(inner)
            def _():
                for which in range(2):
                    each(1, half, lambda i: relay_copy(i, which).wait_send())

    else:
        send_pre, recv_pre, pre_send_sem, pre_recv_sem = exchange

        def pre_copy(step):
            return remote(
                send_pre.at[peer(step)],
                recv_pre.at[me],
                pre_send_sem.at[step],
                pre_recv_sem.at[me],
                peer(step),
            )

        each(0, n, fill_new)
        recv_new[me] = send_new[me]
        prefix[...] = jnp.zeros_like(prefix)
        early = min(EARLY, n - 1) + 1
        each(1, early, lambda step: new_to(peer(step)).start())
        loads[2].wait()
        loads[3].wait()
        read_tables()

        def fill_pre(target):
            slot = jnp.maximum(wanted(target, me), 0)
            for side in range(2):
                send_pre[target, side] = pool[side, slot]

        fill_pre(peer(1))

        def pipelined(step):
            fill_pre(peer(step))
            pre_copy(step - 1).start()

        each(2, n, pipelined)
        fill_pre(me)
        pre_copy(n - 1).start()
        recv_pre[me] = send_pre[me]
        each(early, n, lambda step: new_to(peer(step)).start())
        index_incoming()
        loads[4].wait()

        each(1, n, lambda step: arrival(step, recv_pre, pre_recv_sem).wait())
        for j in range(prefix_pages):
            for side in range(2):
                prefix[side, j * page_rows : (j + 1) * page_rows, :] = recv_pre[
                    page_holder[0, j], side
                ]

        def sent_pages():
            each(1, n, lambda step: pre_copy(step).wait_send())

    factor = math.log2(math.e) / math.sqrt(HEAD)
    nt = (((1,), (1,)), ((), ()))
    row_pos = lax.rem(lax.broadcasted_iota(jnp.int32, (group * ROWS, ROWS), 0), ROWS)
    col_pos = lax.broadcasted_iota(jnp.int32, (group * ROWS, ROWS), 1)
    prefix_pos = lax.broadcasted_iota(jnp.int32, (group * ROWS, prefix.shape[1]), 1)
    prefix_tokens = prefix_len[0]

    def head_cols(g, h):
        return pl.ds(pl.multiple_of((g * group + h) * HEAD, HEAD), HEAD)

    def attend(g):
        kv_cols = pl.ds(pl.multiple_of(g * HEAD, HEAD), HEAD)
        for block in range(span // ROWS):
            rows = slice(block * ROWS, (block + 1) * ROWS)
            keys = (block + 1) * ROWS
            query = jnp.concatenate(
                [q[rows, head_cols(g, h)] for h in range(group)], axis=0
            )
            old = lax.dot_general(
                query, prefix[0, :, kv_cols], nt, preferred_element_type=jnp.float32
            )
            fresh = lax.dot_general(
                query,
                kv[0, : keys // page_rows, :, kv_cols].reshape(keys, HEAD),
                nt,
                preferred_element_type=jnp.float32,
            )
            old = jnp.where(prefix_pos < prefix_tokens, old, -jnp.inf)
            last = jnp.where(col_pos <= row_pos, fresh[:, block * ROWS :], -jnp.inf)
            parts = [fresh[:, i * ROWS : (i + 1) * ROWS] for i in range(block)] + [last]
            top = old
            for part in parts:
                top = jnp.maximum(top, part)
            top = jnp.max(top, axis=1, keepdims=True)
            old = jnp.exp2((old - top) * factor)
            parts = [jnp.exp2((part - top) * factor) for part in parts]
            total = old
            for part in parts:
                total = total + part
            total = jnp.sum(total, axis=1, keepdims=True)
            weighted = jnp.dot(
                old.astype(jnp.bfloat16),
                prefix[1, :, kv_cols],
                preferred_element_type=jnp.float32,
            )
            weighted = weighted + jnp.dot(
                jnp.concatenate(parts, axis=1).astype(jnp.bfloat16),
                kv[1, : keys // page_rows, :, kv_cols].reshape(keys, HEAD),
                preferred_element_type=jnp.float32,
            )
            result = weighted * (1.0 / total)
            result = jnp.where(row_pos + block * ROWS < live, result, 0.0).astype(jnp.bfloat16)
            for h in range(group):
                out[rows, head_cols(g, h)] = result[h * ROWS : (h + 1) * ROWS]

    each(0, KV_HEADS, attend)

    each(1, n, lambda step: arrival(step, recv_new, new_recv_sem).wait())

    def place_page(slot):
        device = source[slot]
        for side in range(2):
            pool_out[side, slot] = jnp.where(
                device >= 0, recv_new[jnp.maximum(device, 0), side], pool[side, slot]
            )

    each(0, slots, place_page)
    each(1, n, lambda step: meta_copy(step).wait_send())
    each(1, n, lambda step: new_to(peer(step)).wait_send())
    sent_pages()


def finish(out, pool_out, o_hbm, pko_hbm, pvo_hbm, sem):
    stores = [
        pltpu.make_async_copy(pool_out.at[0], pko_hbm, sem.at[1]),
        pltpu.make_async_copy(pool_out.at[1], pvo_hbm, sem.at[2]),
        pltpu.make_async_copy(out, o_hbm, sem.at[0]),
    ]
    for store in stores:
        store.start()
    for store in stores:
        store.wait()


def shards(
    queries,
    new_keys,
    new_values,
    pool_keys,
    pool_values,
    prefix_len,
    new_len,
    page_holder,
    page_slot,
    new_holder,
    new_slot,
):
    n = lax.axis_size("seq")
    slots, page_rows, width = pool_keys.shape
    span = queries.shape[0]
    new_pages = new_holder.shape[1]
    prefix_pages = page_holder.shape[1]
    padded = -(-prefix_pages * page_rows // ROWS) * ROWS
    kind = queries.dtype
    tables = (prefix_len, new_len, page_holder, page_slot, new_holder, new_slot)
    anywhere = pl.BlockSpec(memory_space=pl.ANY)
    peers = pltpu.SemaphoreType.DMA((n,))

    def pages(*count):
        return pltpu.VMEM((*count, page_rows, width), kind)

    if crosses_once(n, new_pages):
        half, plane, left = n // 2, n // 4, slots - new_pages
        exchange = [
            pages(left),
            pages(left),
            pages(2, left),
            pages(2, left),
            pages(half, 2),
            pages(half, 2),
            pages(half, 2),
            pages(half, 2),
            pages(plane, 2),
            pages(plane, 2),
            pltpu.SMEM((n,), jnp.int32),
            pltpu.SemaphoreType.DMA((2,)),
            pltpu.SemaphoreType.DMA((2, 2)),
            pltpu.SemaphoreType.DMA((half,)),
            pltpu.SemaphoreType.DMA((half,)),
            pltpu.SemaphoreType.DMA((half, 2)),
            pltpu.SemaphoreType.DMA((plane, 2)),
        ]
    else:
        exchange = [pages(n, 2), pages(n, 2), peers, peers]
    held = pl.BlockSpec(memory_space=pltpu.VMEM)
    page_bytes = 2 * page_rows * width * kind.itemsize
    kept = queries.size * kind.itemsize + slots * page_bytes
    grant = 67043328 - kept - 256 * 1024
    results = (
        jax.ShapeDtypeStruct(queries.shape, kind),
        jax.ShapeDtypeStruct(pool_keys.shape, kind),
        jax.ShapeDtypeStruct(pool_values.shape, kind),
    )
    out, pool_out = pl.pallas_call(
        functools.partial(kernel, n, new_pages, prefix_pages),
        out_shape=(
            pltpu.VMEM(queries.shape, kind),
            pltpu.VMEM((2, slots, page_rows, width), kind),
        ),
        in_specs=[anywhere] * 11,
        out_specs=(held, held),
        scratch_shapes=[
            pages(n, 2),
            pages(2, slots),
            pltpu.SMEM((slots,), jnp.int32),
            *[pltpu.SMEM(table.shape, table.dtype) for table in tables],
            pltpu.VMEM(queries.shape, kind),
            pltpu.VMEM((2, span // page_rows, page_rows, width), kind),
            pltpu.VMEM((2, padded, width), kind),
            pages(n, 2),
            pltpu.VMEM((1, 128), jnp.int32),
            pltpu.VMEM((n, 1, 128), jnp.int32),
            pltpu.SMEM((n, 1, 128), jnp.int32),
            pltpu.SemaphoreType.DMA((5,)),
            pltpu.SemaphoreType.DMA((len(tables),)),
            pltpu.SemaphoreType.DMA,
            peers,
            peers,
            peers,
            peers,
            *exchange,
        ],
        compiler_params=pltpu.CompilerParams(
            collective_id=0, has_side_effects=True, vmem_limit_bytes=grant
        ),
    )(
        *tables,
        queries,
        new_keys.reshape(span // page_rows, page_rows, width),
        new_values.reshape(span // page_rows, page_rows, width),
        pool_keys,
        pool_values,
    )
    return pl.pallas_call(
        finish,
        out_shape=results,
        in_specs=[held, held],
        out_specs=(anywhere,) * 3,
        scratch_shapes=[pltpu.SemaphoreType.DMA((3,))],
        compiler_params=pltpu.CompilerParams(vmem_limit_bytes=1024 * 1024),
    )(out, pool_out)


def solution(mesh):
    rows = P(("groups", "seq"), None)
    pages = P(("groups", "seq"), None, None)
    each = P(("groups", "seq"))
    return jax.shard_map(
        shards,
        mesh=mesh,
        in_specs=(rows, rows, rows, pages, pages, each, each, rows, rows, rows, rows),
        out_specs=(rows, pages, pages),
        check_vma=False,
    )
```

```python
import functools
import math

import jax
import jax.numpy as jnp
from jax import lax
from jax.experimental import pallas as pl
from jax.experimental.pallas import tpu as pltpu
from jax.sharding import PartitionSpec as P

HEADS = 32
KV_HEADS = 8
HEAD = 128
ROWS = 128
SLOT_LANE = 64
EARLY = 5
INNER = (
    (("far", 0), ("far", 1)),
    (
        ("beside", 3),
        ("own", 0),
        ("mirror", 0),
        ("layer", 1),
        ("layer", 2),
        ("layer", 3),
        ("beside", 1),
        ("far", 2),
        ("mirror", 1),
        ("near", 1),
        ("near", 2),
        ("far", 3),
        ("beside", 2),
        ("relay", 0),
        ("relay", 1),
        ("near", 3),
    ),
    (("beside", 0), ("near", 0)),
)
OUTER = (
    (("beside", 2), ("far", 1), ("far", 2)),
    (
        ("own", 0),
        ("mirror", 0),
        ("mirror", 1),
        ("beside", 0),
        ("beside", 3),
        ("beside", 1),
        ("near", 0),
        ("near", 3),
        ("near", 1),
        ("near", 2),
        ("far", 3),
        ("layer", 1),
        ("layer", 2),
        ("layer", 3),
    ),
    (("far", 0),),
)
MESH = pl.DeviceIdType.MESH


def crosses_once(n, new_pages):
    return n == new_pages and n % 4 == 0


def kernel(
    n,
    new_pages,
    prefix_pages,
    prefix_len_hbm,
    new_len_hbm,
    page_holder_hbm,
    page_slot_hbm,
    new_holder_hbm,
    new_slot_hbm,
    q_hbm,
    k_hbm,
    v_hbm,
    pk_hbm,
    pv_hbm,
    out,
    pool_out,
    recv_new,
    pool,
    source,
    prefix_len,
    new_len,
    page_holder,
    page_slot,
    new_holder,
    new_slot,
    q,
    kv,
    prefix,
    send_new,
    meta,
    recv_meta,
    tables,
    in_sem,
    own_sem,
    table_sem,
    meta_send_sem,
    meta_recv_sem,
    new_send_sem,
    new_recv_sem,
    *exchange,
):
    me = lax.axis_index("seq")
    mine = lax.axis_index("groups")
    halves = crosses_once(n, new_pages)
    span = q.shape[0]
    page_rows = pool.shape[2]
    slots = pool.shape[1]
    group = HEADS // KV_HEADS

    def peer(step):
        return lax.rem(me + step, n)

    barrier = pltpu.get_barrier_semaphore()

    def greet(step, carry):
        pl.semaphore_signal(barrier, inc=1, device_id=(mine, peer(step)), device_id_type=MESH)
        return carry

    lax.fori_loop(1, n, greet, 0)

    given = [
        pltpu.make_async_copy(there, here, own_sem.at[i])
        for i, (there, here) in enumerate(
            (
                (new_holder_hbm, new_holder),
                (new_slot_hbm, new_slot),
                (page_holder_hbm, page_holder),
                (page_slot_hbm, page_slot),
                (new_len_hbm, new_len),
                (prefix_len_hbm, prefix_len),
            )
        )
    ]
    for copy in given:
        copy.start()
    loads = [
        pltpu.make_async_copy(k_hbm, kv.at[0], in_sem.at[0]),
        pltpu.make_async_copy(v_hbm, kv.at[1], in_sem.at[1]),
        pltpu.make_async_copy(pk_hbm, pool.at[0], in_sem.at[2]),
        pltpu.make_async_copy(pv_hbm, pool.at[1], in_sem.at[3]),
        pltpu.make_async_copy(q_hbm, q, in_sem.at[4]),
    ]
    for load in loads:
        load.start()

    for copy in given:
        copy.wait()

    lanes = lax.broadcasted_iota(jnp.int32, meta.shape, 1)
    row = jnp.full(meta.shape, -1, jnp.int32)
    for i in range(new_pages):
        row = jnp.where(lanes == i, new_holder[0, i], row)
        row = jnp.where(lanes == SLOT_LANE + i, new_slot[0, i], row)
    for j in range(prefix_pages):
        row = jnp.where(lanes == new_pages + j, page_holder[0, j], row)
        row = jnp.where(lanes == SLOT_LANE + new_pages + j, page_slot[0, j], row)
    meta[...] = row
    recv_meta[me] = row

    live = new_len[0]
    page_pos = lax.broadcasted_iota(jnp.int32, (page_rows, kv.shape[3]), 0)

    def fill_new(target):
        page = jnp.int32(0)
        for i in range(new_pages):
            page = jnp.where(new_holder[0, i] == target, i, page)
        keep = page_pos < live - page * page_rows
        for side in range(2):
            rows = kv[side, page]
            send_new[target, side] = jnp.where(keep, rows, jnp.zeros_like(rows))

    def remote(sent, received, send_sem, recv_sem, target):
        return pltpu.make_async_remote_copy(
            src_ref=sent,
            dst_ref=received,
            send_sem=send_sem,
            recv_sem=recv_sem,
            device_id=(mine, target),
            device_id_type=MESH,
        )

    def landed(buffer, sem):
        return pltpu.make_async_copy(buffer, buffer, sem)

    def meta_copy(step):
        return remote(
            meta, recv_meta.at[me], meta_send_sem.at[step], meta_recv_sem.at[me], peer(step)
        )

    def new_to(target):
        return remote(
            send_new.at[target],
            recv_new.at[me],
            new_send_sem.at[target],
            new_recv_sem.at[me],
            target,
        )

    def arrival(step, buffer, sem):
        at = peer(step)
        return landed(buffer.at[at], sem.at[at])

    pl.semaphore_wait(barrier, n - 1)

    def each(first, last, act):
        def body(step, carry):
            act(step)
            return carry

        lax.fori_loop(first, last, body, 0)

    each(1, n, lambda step: meta_copy(step).start())
    loads[0].wait()
    loads[1].wait()

    def wanted(conversation, holder):
        slot = jnp.int32(-1)
        for j in range(prefix_pages):
            slot = jnp.where(
                tables[conversation, 0, new_pages + j] == holder,
                tables[conversation, 0, SLOT_LANE + new_pages + j],
                slot,
            )
        return slot

    def read_tables():
        each(1, n, lambda step: arrival(step, recv_meta, meta_recv_sem).wait())
        table_copy = pltpu.make_async_copy(recv_meta, tables, table_sem)
        table_copy.start()
        table_copy.wait()

    def index_incoming():
        def clear(slot):
            source[slot] = -1

        each(0, slots, clear)

        def incoming(device):
            landing = jnp.int32(-1)
            for i in range(new_pages):
                landing = jnp.where(
                    tables[device, 0, i] == me, tables[device, 0, SLOT_LANE + i], landing
                )

            for slot in range(slots):
                source[slot] = jnp.where(landing == slot, device, source[slot])

        each(0, n, incoming)

    if halves:
        (
            mirror_k,
            mirror_v,
            mirrored_k,
            mirrored_v,
            send_own,
            recv_own,
            relay_k,
            relay_v,
            recv_k,
            recv_v,
            ranks,
            mirror_send_sem,
            mirror_recv_sem,
            own_send_sem,
            own_recv_sem,
            relay_send_sem,
            relay_recv_sem,
        ) = exchange
        half, plane = n // 2, n // 4
        layer, place = me // plane, lax.rem(me, plane)
        mine_half = me // half
        base, other = mine_half * half, (1 - mine_half) * half
        inner = (layer == 1) | (layer == 2)
        here = me - base
        kept = mirror_k.shape[0]

        def in_layer(which, i):
            return which * plane + lax.rem(place + i, plane)

        layers = {
            "layer": layer,
            "beside": base // plane + 1 - lax.rem(layer, 2),
            "near": 2 - mine_half,
            "far": 3 - 3 * mine_half,
        }

        def target(which, i):
            return in_layer(layers[which], i)

        def early_fill(order):
            for which, i in order[0]:
                fill_new(target(which, i))

        def late_fill(order):
            for which, i in order[1] + order[2]:
                if which in layers:
                    fill_new(target(which, i))

        def stage(order, number):
            for which, i in order[number]:
                if which == "own":
                    each(1, half, lambda j: own_copy(j).start())
                elif which == "mirror":
                    mirror_copy(i).start()
                elif which == "relay":
                    forward(i)
                else:
                    new_to(target(which, i)).start()

        def by_layer(act):
            pl.when(inner)(functools.partial(act, INNER))
            pl.when(jnp.logical_not(inner))(functools.partial(act, OUTER))

        mirror_at = half - plane * mine_half + place
        origin = lax.rem(layer, 2)

        def mirror_copy(which):
            sent, received = ((mirror_k, mirrored_k), (mirror_v, mirrored_v))[which]
            return remote(
                sent,
                received.at[origin],
                mirror_send_sem.at[which],
                mirror_recv_sem.at[origin, which],
                mirror_at,
            )

        def half_peer(i):
            return lax.rem(here + i, half)

        def own_copy(i):
            to = half_peer(i)
            return remote(
                send_own.at[to],
                recv_own.at[here],
                own_send_sem.at[to],
                own_recv_sem.at[here],
                base + to,
            )

        def relay_copy(i, which):
            to = half_peer(i)
            sent, received = ((relay_k, recv_k), (relay_v, recv_v))[which]
            return remote(
                sent.at[to],
                received.at[place],
                relay_send_sem.at[to, which],
                relay_recv_sem.at[place, which],
                base + to,
            )

        def forward(which):
            sent, got = ((relay_k, mirrored_k), (relay_v, mirrored_v))[which]
            received = (recv_k, recv_v)[which]
            for o in range(2):
                landed(got.at[o], mirror_recv_sem.at[o, which]).wait()

            def fill_relay(i):
                to = half_peer(i)
                for o in range(2):
                    sent[to, o] = got[o, ranks[to * 2 + o]]

            fill_relay(1)

            def relay_step(i):
                fill_relay(i)
                relay_copy(i - 1, which).start()

            each(2, half, relay_step)
            fill_relay(0)
            relay_copy(half - 1, which).start()
            received[place] = sent[here]

        by_layer(early_fill)
        by_layer(lambda order: stage(order, 0))
        by_layer(late_fill)
        fill_new(me)
        recv_new[me] = send_new[me]
        prefix[...] = jnp.zeros_like(prefix)
        loads[2].wait()
        loads[3].wait()
        read_tables()

        def pick(i, carry):
            count, picks = carry
            slot = wanted(other + i, me)
            found = slot >= 0
            picks = tuple(
                jnp.where(found & (count == k), slot, p) for k, p in enumerate(picks)
            )
            return count + jnp.where(found, 1, 0), picks

        picks = lax.fori_loop(
            0, half, pick, (jnp.int32(0), (jnp.int32(0),) * kept)
        )[1]
        for k in range(kept):
            mirror_k[k] = pool[0, picks[k]]
        for k in range(kept):
            mirror_v[k] = pool[1, picks[k]]

        def fill_own(to):
            slot = jnp.maximum(wanted(base + to, me), 0)
            for side in range(2):
                send_own[to, side] = pool[side, slot]

        each(0, half, fill_own)

        for o in range(2):
            def rank(i, count):
                ranks[i * 2 + o] = jnp.minimum(count, kept - 1)
                found = wanted(base + i, other + o * plane + place) >= 0
                return count + jnp.where(found, 1, 0)

            lax.fori_loop(0, half, rank, jnp.int32(0))

        by_layer(lambda order: stage(order, 1))
        recv_own[here] = send_own[here]
        index_incoming()
        loads[4].wait()

        each(1, half, lambda i: landed(
            recv_own.at[half_peer(i)], own_recv_sem.at[half_peer(i)]
        ).wait())
        for which in range(2):
            received = (recv_k, recv_v)[which]

            def relayed(i):
                @pl.when(jnp.logical_not(inner & (i == place)))
                def _():
                    landed(received.at[i], relay_recv_sem.at[i, which]).wait()

            each(0, plane, relayed)

        by_layer(lambda order: stage(order, 2))

        for j in range(prefix_pages):
            holder = page_holder[0, j]
            close = holder // half == mine_half
            for side in range(2):
                own = recv_own[lax.rem(holder, half), side]
                through = (recv_k, recv_v)[side][
                    lax.rem(holder, plane), lax.rem(holder // plane, 2)
                ]
                prefix[side, j * page_rows : (j + 1) * page_rows, :] = jnp.where(
                    close, own, through
                )

        def sent_pages():
            mirror_copy(0).wait_send()
            mirror_copy(1).wait_send()
            each(1, half, lambda i: own_copy(i).wait_send())

            @pl.when(inner)
            def _():
                for which in range(2):
                    each(1, half, lambda i: relay_copy(i, which).wait_send())

    else:
        send_pre, recv_pre, pre_send_sem, pre_recv_sem = exchange

        def pre_copy(step):
            return remote(
                send_pre.at[peer(step)],
                recv_pre.at[me],
                pre_send_sem.at[step],
                pre_recv_sem.at[me],
                peer(step),
            )

        each(0, n, fill_new)
        recv_new[me] = send_new[me]
        prefix[...] = jnp.zeros_like(prefix)
        early = min(EARLY, n - 1) + 1
        each(1, early, lambda step: new_to(peer(step)).start())
        loads[2].wait()
        loads[3].wait()
        read_tables()

        def fill_pre(target):
            slot = jnp.maximum(wanted(target, me), 0)
            for side in range(2):
                send_pre[target, side] = pool[side, slot]

        fill_pre(peer(1))

        def pipelined(step):
            fill_pre(peer(step))
            pre_copy(step - 1).start()

        each(2, n, pipelined)
        fill_pre(me)
        pre_copy(n - 1).start()
        recv_pre[me] = send_pre[me]
        each(early, n, lambda step: new_to(peer(step)).start())
        index_incoming()
        loads[4].wait()

        each(1, n, lambda step: arrival(step, recv_pre, pre_recv_sem).wait())
        for j in range(prefix_pages):
            for side in range(2):
                prefix[side, j * page_rows : (j + 1) * page_rows, :] = recv_pre[
                    page_holder[0, j], side
                ]

        def sent_pages():
            each(1, n, lambda step: pre_copy(step).wait_send())

    factor = math.log2(math.e) / math.sqrt(HEAD)
    nt = (((1,), (1,)), ((), ()))
    row_pos = lax.rem(lax.broadcasted_iota(jnp.int32, (group * ROWS, ROWS), 0), ROWS)
    col_pos = lax.broadcasted_iota(jnp.int32, (group * ROWS, ROWS), 1)
    prefix_pos = lax.broadcasted_iota(jnp.int32, (group * ROWS, prefix.shape[1]), 1)
    prefix_tokens = prefix_len[0]

    def head_cols(g, h):
        return pl.ds(pl.multiple_of((g * group + h) * HEAD, HEAD), HEAD)

    def attend(g):
        kv_cols = pl.ds(pl.multiple_of(g * HEAD, HEAD), HEAD)
        for block in range(span // ROWS):
            rows = slice(block * ROWS, (block + 1) * ROWS)
            keys = (block + 1) * ROWS
            query = jnp.concatenate(
                [q[rows, head_cols(g, h)] for h in range(group)], axis=0
            )
            old = lax.dot_general(
                query, prefix[0, :, kv_cols], nt, preferred_element_type=jnp.float32
            )
            fresh = lax.dot_general(
                query,
                kv[0, : keys // page_rows, :, kv_cols].reshape(keys, HEAD),
                nt,
                preferred_element_type=jnp.float32,
            )
            old = jnp.where(prefix_pos < prefix_tokens, old, -jnp.inf)
            last = jnp.where(col_pos <= row_pos, fresh[:, block * ROWS :], -jnp.inf)
            parts = [fresh[:, i * ROWS : (i + 1) * ROWS] for i in range(block)] + [last]
            top = old
            for part in parts:
                top = jnp.maximum(top, part)
            top = jnp.max(top, axis=1, keepdims=True)
            old = jnp.exp2((old - top) * factor)
            parts = [jnp.exp2((part - top) * factor) for part in parts]
            total = old
            for part in parts:
                total = total + part
            total = jnp.sum(total, axis=1, keepdims=True)
            weighted = jnp.dot(
                old.astype(jnp.bfloat16),
                prefix[1, :, kv_cols],
                preferred_element_type=jnp.float32,
            )
            weighted = weighted + jnp.dot(
                jnp.concatenate(parts, axis=1).astype(jnp.bfloat16),
                kv[1, : keys // page_rows, :, kv_cols].reshape(keys, HEAD),
                preferred_element_type=jnp.float32,
            )
            result = weighted * (1.0 / total)
            result = jnp.where(row_pos + block * ROWS < live, result, 0.0).astype(jnp.bfloat16)
            for h in range(group):
                out[rows, head_cols(g, h)] = result[h * ROWS : (h + 1) * ROWS]

    each(0, KV_HEADS, attend)

    each(1, n, lambda step: arrival(step, recv_new, new_recv_sem).wait())

    def place_page(slot):
        device = source[slot]
        for side in range(2):
            pool_out[side, slot] = jnp.where(
                device >= 0, recv_new[jnp.maximum(device, 0), side], pool[side, slot]
            )

    each(0, slots, place_page)
    each(1, n, lambda step: meta_copy(step).wait_send())
    each(1, n, lambda step: new_to(peer(step)).wait_send())
    sent_pages()


def finish(out, pool_out, o_hbm, pko_hbm, pvo_hbm, sem):
    stores = [
        pltpu.make_async_copy(pool_out.at[0], pko_hbm, sem.at[1]),
        pltpu.make_async_copy(pool_out.at[1], pvo_hbm, sem.at[2]),
        pltpu.make_async_copy(out, o_hbm, sem.at[0]),
    ]
    for store in stores:
        store.start()
    for store in stores:
        store.wait()


def shards(
    queries,
    new_keys,
    new_values,
    pool_keys,
    pool_values,
    prefix_len,
    new_len,
    page_holder,
    page_slot,
    new_holder,
    new_slot,
):
    n = lax.axis_size("seq")
    slots, page_rows, width = pool_keys.shape
    span = queries.shape[0]
    new_pages = new_holder.shape[1]
    prefix_pages = page_holder.shape[1]
    padded = -(-prefix_pages * page_rows // ROWS) * ROWS
    kind = queries.dtype
    tables = (prefix_len, new_len, page_holder, page_slot, new_holder, new_slot)
    anywhere = pl.BlockSpec(memory_space=pl.ANY)
    peers = pltpu.SemaphoreType.DMA((n,))

    def pages(*count):
        return pltpu.VMEM((*count, page_rows, width), kind)

    if crosses_once(n, new_pages):
        half, plane, left = n // 2, n // 4, slots - new_pages
        exchange = [
            pages(left),
            pages(left),
            pages(2, left),
            pages(2, left),
            pages(half, 2),
            pages(half, 2),
            pages(half, 2),
            pages(half, 2),
            pages(plane, 2),
            pages(plane, 2),
            pltpu.SMEM((n,), jnp.int32),
            pltpu.SemaphoreType.DMA((2,)),
            pltpu.SemaphoreType.DMA((2, 2)),
            pltpu.SemaphoreType.DMA((half,)),
            pltpu.SemaphoreType.DMA((half,)),
            pltpu.SemaphoreType.DMA((half, 2)),
            pltpu.SemaphoreType.DMA((plane, 2)),
        ]
    else:
        exchange = [pages(n, 2), pages(n, 2), peers, peers]
    held = pl.BlockSpec(memory_space=pltpu.VMEM)
    page_bytes = 2 * page_rows * width * kind.itemsize
    kept = queries.size * kind.itemsize + slots * page_bytes
    grant = 67043328 - kept - 256 * 1024
    results = (
        jax.ShapeDtypeStruct(queries.shape, kind),
        jax.ShapeDtypeStruct(pool_keys.shape, kind),
        jax.ShapeDtypeStruct(pool_values.shape, kind),
    )
    out, pool_out = pl.pallas_call(
        functools.partial(kernel, n, new_pages, prefix_pages),
        out_shape=(
            pltpu.VMEM(queries.shape, kind),
            pltpu.VMEM((2, slots, page_rows, width), kind),
        ),
        in_specs=[anywhere] * 11,
        out_specs=(held, held),
        scratch_shapes=[
            pages(n, 2),
            pages(2, slots),
            pltpu.SMEM((slots,), jnp.int32),
            *[pltpu.SMEM(table.shape, table.dtype) for table in tables],
            pltpu.VMEM(queries.shape, kind),
            pltpu.VMEM((2, span // page_rows, page_rows, width), kind),
            pltpu.VMEM((2, padded, width), kind),
            pages(n, 2),
            pltpu.VMEM((1, 128), jnp.int32),
            pltpu.VMEM((n, 1, 128), jnp.int32),
            pltpu.SMEM((n, 1, 128), jnp.int32),
            pltpu.SemaphoreType.DMA((5,)),
            pltpu.SemaphoreType.DMA((len(tables),)),
            pltpu.SemaphoreType.DMA,
            peers,
            peers,
            peers,
            peers,
            *exchange,
        ],
        compiler_params=pltpu.CompilerParams(
            collective_id=0, has_side_effects=True, vmem_limit_bytes=grant
        ),
    )(
        *tables,
        queries,
        new_keys.reshape(span // page_rows, page_rows, width),
        new_values.reshape(span // page_rows, page_rows, width),
        pool_keys,
        pool_values,
    )
    return pl.pallas_call(
        finish,
        out_shape=results,
        in_specs=[held, held],
        out_specs=(anywhere,) * 3,
        scratch_shapes=[pltpu.SemaphoreType.DMA((3,))],
        compiler_params=pltpu.CompilerParams(vmem_limit_bytes=1024 * 1024),
    )(out, pool_out)


def solution(mesh):
    rows = P(("groups", "seq"), None)
    pages = P(("groups", "seq"), None, None)
    each = P(("groups", "seq"))
    return jax.shard_map(
        shards,
        mesh=mesh,
        in_specs=(rows, rows, rows, pages, pages, each, each, rows, rows, rows, rows),
        out_specs=(rows, pages, pages),
        check_vma=False,
    )
```

```python
import functools
import math

import jax
import jax.numpy as jnp
from jax import lax
from jax.experimental import pallas as pl
from jax.experimental.pallas import tpu as pltpu
from jax.sharding import PartitionSpec as P

HEADS = 32
KV_HEADS = 8
HEAD = 128
ROWS = 128
SLOT_LANE = 64
EARLY = 5
INNER = (
    (("far", 0), ("far", 1)),
    (
        ("beside", 3),
        ("own", 0),
        ("mirror", 0),
        ("layer", 1),
        ("layer", 2),
        ("layer", 3),
        ("beside", 1),
        ("far", 2),
        ("mirror", 1),
        ("near", 1),
        ("near", 2),
        ("far", 3),
        ("beside", 2),
        ("relay", 0),
        ("relay", 1),
        ("near", 3),
    ),
    (("beside", 0), ("near", 0)),
)
OUTER = (
    (("beside", 2), ("far", 1), ("far", 2)),
    (
        ("own", 0),
        ("mirror", 0),
        ("mirror", 1),
        ("beside", 0),
        ("beside", 3),
        ("beside", 1),
        ("near", 0),
        ("near", 3),
        ("near", 1),
        ("near", 2),
        ("far", 3),
        ("layer", 1),
        ("layer", 2),
        ("layer", 3),
    ),
    (("far", 0),),
)
MESH = pl.DeviceIdType.MESH


def crosses_once(n, new_pages):
    return n == new_pages and n % 4 == 0


def kernel(
    n,
    new_pages,
    prefix_pages,
    prefix_len_hbm,
    new_len_hbm,
    page_holder_hbm,
    page_slot_hbm,
    new_holder_hbm,
    new_slot_hbm,
    q_hbm,
    k_hbm,
    v_hbm,
    pk_hbm,
    pv_hbm,
    out,
    recv_new,
    pool,
    source,
    prefix_len,
    new_len,
    page_holder,
    page_slot,
    new_holder,
    new_slot,
    q,
    kv,
    prefix,
    send_new,
    meta,
    recv_meta,
    tables,
    in_sem,
    own_sem,
    table_sem,
    meta_send_sem,
    meta_recv_sem,
    new_send_sem,
    new_recv_sem,
    *exchange,
):
    me = lax.axis_index("seq")
    mine = lax.axis_index("groups")
    halves = crosses_once(n, new_pages)
    span = q.shape[0]
    page_rows = pool.shape[2]
    slots = pool.shape[1]
    group = HEADS // KV_HEADS

    def peer(step):
        return lax.rem(me + step, n)

    barrier = pltpu.get_barrier_semaphore()

    def greet(step, carry):
        pl.semaphore_signal(barrier, inc=1, device_id=(mine, peer(step)), device_id_type=MESH)
        return carry

    lax.fori_loop(1, n, greet, 0)

    given = [
        pltpu.make_async_copy(there, here, own_sem.at[i])
        for i, (there, here) in enumerate(
            (
                (new_holder_hbm, new_holder),
                (new_slot_hbm, new_slot),
                (page_holder_hbm, page_holder),
                (page_slot_hbm, page_slot),
                (new_len_hbm, new_len),
                (prefix_len_hbm, prefix_len),
            )
        )
    ]
    for copy in given:
        copy.start()
    loads = [
        pltpu.make_async_copy(k_hbm, kv.at[0], in_sem.at[0]),
        pltpu.make_async_copy(v_hbm, kv.at[1], in_sem.at[1]),
        pltpu.make_async_copy(pk_hbm, pool.at[0], in_sem.at[2]),
        pltpu.make_async_copy(pv_hbm, pool.at[1], in_sem.at[3]),
        pltpu.make_async_copy(q_hbm, q, in_sem.at[4]),
    ]
    for load in loads:
        load.start()

    for copy in given:
        copy.wait()

    lanes = lax.broadcasted_iota(jnp.int32, meta.shape, 1)
    row = jnp.full(meta.shape, -1, jnp.int32)
    for i in range(new_pages):
        row = jnp.where(lanes == i, new_holder[0, i], row)
        row = jnp.where(lanes == SLOT_LANE + i, new_slot[0, i], row)
    for j in range(prefix_pages):
        row = jnp.where(lanes == new_pages + j, page_holder[0, j], row)
        row = jnp.where(lanes == SLOT_LANE + new_pages + j, page_slot[0, j], row)
    meta[...] = row
    recv_meta[me] = row

    live = new_len[0]
    page_pos = lax.broadcasted_iota(jnp.int32, (page_rows, kv.shape[3]), 0)

    def fill_new(target):
        page = jnp.int32(0)
        for i in range(new_pages):
            page = jnp.where(new_holder[0, i] == target, i, page)
        keep = page_pos < live - page * page_rows
        for side in range(2):
            rows = kv[side, page]
            send_new[target, side] = jnp.where(keep, rows, jnp.zeros_like(rows))

    def remote(sent, received, send_sem, recv_sem, target):
        return pltpu.make_async_remote_copy(
            src_ref=sent,
            dst_ref=received,
            send_sem=send_sem,
            recv_sem=recv_sem,
            device_id=(mine, target),
            device_id_type=MESH,
        )

    def landed(buffer, sem):
        return pltpu.make_async_copy(buffer, buffer, sem)

    def meta_copy(step):
        return remote(
            meta, recv_meta.at[me], meta_send_sem.at[step], meta_recv_sem.at[me], peer(step)
        )

    def new_to(target):
        return remote(
            send_new.at[target],
            recv_new.at[me],
            new_send_sem.at[target],
            new_recv_sem.at[me],
            target,
        )

    def arrival(step, buffer, sem):
        at = peer(step)
        return landed(buffer.at[at], sem.at[at])

    pl.semaphore_wait(barrier, n - 1)

    def each(first, last, act):
        def body(step, carry):
            act(step)
            return carry

        lax.fori_loop(first, last, body, 0)

    each(1, n, lambda step: meta_copy(step).start())
    loads[0].wait()
    loads[1].wait()

    def wanted(conversation, holder):
        slot = jnp.int32(-1)
        for j in range(prefix_pages):
            slot = jnp.where(
                tables[conversation, 0, new_pages + j] == holder,
                tables[conversation, 0, SLOT_LANE + new_pages + j],
                slot,
            )
        return slot

    def read_tables():
        each(1, n, lambda step: arrival(step, recv_meta, meta_recv_sem).wait())
        table_copy = pltpu.make_async_copy(recv_meta, tables, table_sem)
        table_copy.start()
        table_copy.wait()

    def index_incoming():
        def incoming(device, origins):
            landing = jnp.int32(-1)
            for i in range(new_pages):
                landing = jnp.where(
                    tables[device, 0, i] == me, tables[device, 0, SLOT_LANE + i], landing
                )
            return jnp.where(lanes == landing, device, origins)

        source[...] = lax.fori_loop(0, n, incoming, jnp.full(source.shape, -1, jnp.int32))

    if halves:
        (
            mirror_k,
            mirror_v,
            mirrored_k,
            mirrored_v,
            send_own,
            recv_own,
            relay_k,
            relay_v,
            recv_k,
            recv_v,
            ranks,
            mirror_send_sem,
            mirror_recv_sem,
            own_send_sem,
            own_recv_sem,
            relay_send_sem,
            relay_recv_sem,
        ) = exchange
        half, plane = n // 2, n // 4
        layer, place = me // plane, lax.rem(me, plane)
        mine_half = me // half
        base, other = mine_half * half, (1 - mine_half) * half
        inner = (layer == 1) | (layer == 2)
        here = me - base
        kept = mirror_k.shape[0]

        def in_layer(which, i):
            return which * plane + lax.rem(place + i, plane)

        layers = {
            "layer": layer,
            "beside": base // plane + 1 - lax.rem(layer, 2),
            "near": 2 - mine_half,
            "far": 3 - 3 * mine_half,
        }

        def target(which, i):
            return in_layer(layers[which], i)

        def early_fill(order):
            for which, i in order[0]:
                fill_new(target(which, i))

        def late_fill(order):
            for which, i in order[1] + order[2]:
                if which in layers:
                    fill_new(target(which, i))

        def stage(order, number):
            for which, i in order[number]:
                if which == "own":
                    each(1, half, lambda j: own_copy(j).start())
                elif which == "mirror":
                    mirror_copy(i).start()
                elif which == "relay":
                    forward(i)
                else:
                    new_to(target(which, i)).start()

        def by_layer(act):
            pl.when(inner)(functools.partial(act, INNER))
            pl.when(jnp.logical_not(inner))(functools.partial(act, OUTER))

        mirror_at = half - plane * mine_half + place
        origin = lax.rem(layer, 2)

        def mirror_copy(which):
            sent, received = ((mirror_k, mirrored_k), (mirror_v, mirrored_v))[which]
            return remote(
                sent,
                received.at[origin],
                mirror_send_sem.at[which],
                mirror_recv_sem.at[origin, which],
                mirror_at,
            )

        def half_peer(i):
            away = (i > 0) & (i <= plane)
            which = jnp.where(away, layers["beside"], layer)
            turn = place + jnp.where(away, i - 1, i)
            return which * plane + lax.rem(turn, plane) - base

        def own_copy(i):
            to = half_peer(i)
            return remote(
                send_own.at[to],
                recv_own.at[here],
                own_send_sem.at[to],
                own_recv_sem.at[here],
                base + to,
            )

        def relay_copy(i, which):
            to = half_peer(i)
            sent, received = ((relay_k, recv_k), (relay_v, recv_v))[which]
            return remote(
                sent.at[to],
                received.at[place],
                relay_send_sem.at[to, which],
                relay_recv_sem.at[place, which],
                base + to,
            )

        def forward(which):
            sent, got = ((relay_k, mirrored_k), (relay_v, mirrored_v))[which]
            received = (recv_k, recv_v)[which]
            for o in range(2):
                landed(got.at[o], mirror_recv_sem.at[o, which]).wait()

            def fill_relay(i):
                to = half_peer(i)
                for o in range(2):
                    sent[to, o] = got[o, ranks[to * 2 + o]]

            fill_relay(1)

            def relay_step(i):
                fill_relay(i)
                relay_copy(i - 1, which).start()

            each(2, half, relay_step)
            fill_relay(0)
            relay_copy(half - 1, which).start()
            received[place] = sent[here]

        by_layer(early_fill)
        by_layer(lambda order: stage(order, 0))
        by_layer(late_fill)
        fill_new(me)
        recv_new[me] = send_new[me]
        prefix[...] = jnp.zeros_like(prefix)
        loads[2].wait()
        loads[3].wait()
        read_tables()

        def pick(i, carry):
            count, picks = carry
            slot = wanted(other + i, me)
            found = slot >= 0
            picks = tuple(
                jnp.where(found & (count == k), slot, p) for k, p in enumerate(picks)
            )
            return count + jnp.where(found, 1, 0), picks

        picks = lax.fori_loop(
            0, half, pick, (jnp.int32(0), (jnp.int32(0),) * kept)
        )[1]
        for k in range(kept):
            mirror_k[k] = pool[0, picks[k]]
        for k in range(kept):
            mirror_v[k] = pool[1, picks[k]]

        def fill_own(to):
            slot = jnp.maximum(wanted(base + to, me), 0)
            for side in range(2):
                send_own[to, side] = pool[side, slot]

        each(0, half, fill_own)

        for o in range(2):
            def rank(i, count):
                ranks[i * 2 + o] = jnp.minimum(count, kept - 1)
                found = wanted(base + i, other + o * plane + place) >= 0
                return count + jnp.where(found, 1, 0)

            lax.fori_loop(0, half, rank, jnp.int32(0))

        by_layer(lambda order: stage(order, 1))
        recv_own[here] = send_own[here]
        index_incoming()
        loads[4].wait()

        each(1, half, lambda i: landed(
            recv_own.at[half_peer(i)], own_recv_sem.at[half_peer(i)]
        ).wait())
        for which in range(2):
            received = (recv_k, recv_v)[which]

            def relayed(i):
                @pl.when(jnp.logical_not(inner & (i == place)))
                def _():
                    landed(received.at[i], relay_recv_sem.at[i, which]).wait()

            each(0, plane, relayed)

        by_layer(lambda order: stage(order, 2))

        for j in range(prefix_pages):
            holder = page_holder[0, j]
            close = holder // half == mine_half
            for side in range(2):
                own = recv_own[lax.rem(holder, half), side]
                through = (recv_k, recv_v)[side][
                    lax.rem(holder, plane), lax.rem(holder // plane, 2)
                ]
                prefix[side, j * page_rows : (j + 1) * page_rows, :] = jnp.where(
                    close, own, through
                )

        def sent_pages():
            mirror_copy(0).wait_send()
            mirror_copy(1).wait_send()
            each(1, half, lambda i: own_copy(i).wait_send())

            @pl.when(inner)
            def _():
                for which in range(2):
                    each(1, half, lambda i: relay_copy(i, which).wait_send())

    else:
        send_pre, recv_pre, pre_send_sem, pre_recv_sem = exchange

        def pre_copy(step):
            return remote(
                send_pre.at[peer(step)],
                recv_pre.at[me],
                pre_send_sem.at[step],
                pre_recv_sem.at[me],
                peer(step),
            )

        each(0, n, fill_new)
        recv_new[me] = send_new[me]
        prefix[...] = jnp.zeros_like(prefix)
        early = min(EARLY, n - 1) + 1
        each(1, early, lambda step: new_to(peer(step)).start())
        loads[2].wait()
        loads[3].wait()
        read_tables()

        def fill_pre(target):
            slot = jnp.maximum(wanted(target, me), 0)
            for side in range(2):
                send_pre[target, side] = pool[side, slot]

        fill_pre(peer(1))

        def pipelined(step):
            fill_pre(peer(step))
            pre_copy(step - 1).start()

        each(2, n, pipelined)
        fill_pre(me)
        pre_copy(n - 1).start()
        recv_pre[me] = send_pre[me]
        each(early, n, lambda step: new_to(peer(step)).start())
        index_incoming()
        loads[4].wait()

        each(1, n, lambda step: arrival(step, recv_pre, pre_recv_sem).wait())
        for j in range(prefix_pages):
            for side in range(2):
                prefix[side, j * page_rows : (j + 1) * page_rows, :] = recv_pre[
                    page_holder[0, j], side
                ]

        def sent_pages():
            each(1, n, lambda step: pre_copy(step).wait_send())

    factor = math.log2(math.e) / math.sqrt(HEAD)
    nt = (((1,), (1,)), ((), ()))
    row_pos = lax.rem(lax.broadcasted_iota(jnp.int32, (group * ROWS, ROWS), 0), ROWS)
    col_pos = lax.broadcasted_iota(jnp.int32, (group * ROWS, ROWS), 1)
    prefix_pos = lax.broadcasted_iota(jnp.int32, (group * ROWS, prefix.shape[1]), 1)
    prefix_tokens = prefix_len[0]

    def head_cols(g, h):
        return pl.ds(pl.multiple_of((g * group + h) * HEAD, HEAD), HEAD)

    def attend(g):
        kv_cols = pl.ds(pl.multiple_of(g * HEAD, HEAD), HEAD)
        for block in range(span // ROWS):
            rows = slice(block * ROWS, (block + 1) * ROWS)
            keys = (block + 1) * ROWS
            query = jnp.concatenate(
                [q[rows, head_cols(g, h)] for h in range(group)], axis=0
            )
            old = lax.dot_general(
                query, prefix[0, :, kv_cols], nt, preferred_element_type=jnp.float32
            )
            fresh = lax.dot_general(
                query,
                kv[0, : keys // page_rows, :, kv_cols].reshape(keys, HEAD),
                nt,
                preferred_element_type=jnp.float32,
            )
            old = jnp.where(prefix_pos < prefix_tokens, old, -jnp.inf)
            last = jnp.where(col_pos <= row_pos, fresh[:, block * ROWS :], -jnp.inf)
            parts = [fresh[:, i * ROWS : (i + 1) * ROWS] for i in range(block)] + [last]
            top = old
            for part in parts:
                top = jnp.maximum(top, part)
            top = jnp.max(top, axis=1, keepdims=True)
            old = jnp.exp2((old - top) * factor)
            parts = [jnp.exp2((part - top) * factor) for part in parts]
            total = old
            for part in parts:
                total = total + part
            total = jnp.sum(total, axis=1, keepdims=True)
            weighted = jnp.dot(
                old.astype(jnp.bfloat16),
                prefix[1, :, kv_cols],
                preferred_element_type=jnp.float32,
            )
            weighted = weighted + jnp.dot(
                jnp.concatenate(parts, axis=1).astype(jnp.bfloat16),
                kv[1, : keys // page_rows, :, kv_cols].reshape(keys, HEAD),
                preferred_element_type=jnp.float32,
            )
            result = weighted * (1.0 / total)
            result = jnp.where(row_pos + block * ROWS < live, result, 0.0).astype(jnp.bfloat16)
            for h in range(group):
                out[rows, head_cols(g, h)] = result[h * ROWS : (h + 1) * ROWS]

    each(0, KV_HEADS, attend)

    each(1, n, lambda step: arrival(step, recv_new, new_recv_sem).wait())
    each(1, n, lambda step: meta_copy(step).wait_send())
    each(1, n, lambda step: new_to(peer(step)).wait_send())
    sent_pages()


def finish(out, recv_new, pool, source, o_hbm, pko_hbm, pvo_hbm, origins, origin_sem, sem):
    table = pltpu.make_async_copy(source, origins, origin_sem)
    table.start()
    whole = pltpu.make_async_copy(out, o_hbm, sem.at[0])
    whole.start()
    table.wait()
    targets = (pko_hbm, pvo_hbm)

    def place(slot, carry):
        device = origins[0, slot]

        @pl.when(device >= 0)
        def _():
            for side in range(2):
                pltpu.make_async_copy(
                    recv_new.at[device, side], targets[side].at[slot], sem.at[1 + side]
                ).start()

        @pl.when(device < 0)
        def _():
            for side in range(2):
                pltpu.make_async_copy(
                    pool.at[side, slot], targets[side].at[slot], sem.at[1 + side]
                ).start()

        return carry

    lax.fori_loop(0, pool.shape[1], place, 0)
    for side in range(2):
        pltpu.make_async_copy(pool.at[side], targets[side], sem.at[1 + side]).wait()
    whole.wait()


def shards(
    queries,
    new_keys,
    new_values,
    pool_keys,
    pool_values,
    prefix_len,
    new_len,
    page_holder,
    page_slot,
    new_holder,
    new_slot,
):
    n = lax.axis_size("seq")
    slots, page_rows, width = pool_keys.shape
    span = queries.shape[0]
    new_pages = new_holder.shape[1]
    prefix_pages = page_holder.shape[1]
    padded = -(-prefix_pages * page_rows // ROWS) * ROWS
    kind = queries.dtype
    tables = (prefix_len, new_len, page_holder, page_slot, new_holder, new_slot)
    anywhere = pl.BlockSpec(memory_space=pl.ANY)
    peers = pltpu.SemaphoreType.DMA((n,))

    def pages(*count):
        return pltpu.VMEM((*count, page_rows, width), kind)

    if crosses_once(n, new_pages):
        half, plane, left = n // 2, n // 4, slots - new_pages
        exchange = [
            pages(left),
            pages(left),
            pages(2, left),
            pages(2, left),
            pages(half, 2),
            pages(half, 2),
            pages(half, 2),
            pages(half, 2),
            pages(plane, 2),
            pages(plane, 2),
            pltpu.SMEM((n,), jnp.int32),
            pltpu.SemaphoreType.DMA((2,)),
            pltpu.SemaphoreType.DMA((2, 2)),
            pltpu.SemaphoreType.DMA((half,)),
            pltpu.SemaphoreType.DMA((half,)),
            pltpu.SemaphoreType.DMA((half, 2)),
            pltpu.SemaphoreType.DMA((plane, 2)),
        ]
    else:
        exchange = [pages(n, 2), pages(n, 2), peers, peers]
    held = pl.BlockSpec(memory_space=pltpu.VMEM)
    page_bytes = 2 * page_rows * width * kind.itemsize
    kept = queries.size * kind.itemsize + (n + slots) * page_bytes + 4096
    grant = 67043328 - kept - 256 * 1024
    results = (
        jax.ShapeDtypeStruct(queries.shape, kind),
        jax.ShapeDtypeStruct(pool_keys.shape, kind),
        jax.ShapeDtypeStruct(pool_values.shape, kind),
    )
    out, recv_new, pool, source = pl.pallas_call(
        functools.partial(kernel, n, new_pages, prefix_pages),
        out_shape=(
            pltpu.VMEM(queries.shape, kind),
            pages(n, 2),
            pages(2, slots),
            pltpu.VMEM((1, 128), jnp.int32),
        ),
        in_specs=[anywhere] * 11,
        out_specs=(held,) * 4,
        scratch_shapes=[
            *[pltpu.SMEM(table.shape, table.dtype) for table in tables],
            pltpu.VMEM(queries.shape, kind),
            pltpu.VMEM((2, span // page_rows, page_rows, width), kind),
            pltpu.VMEM((2, padded, width), kind),
            pages(n, 2),
            pltpu.VMEM((1, 128), jnp.int32),
            pltpu.VMEM((n, 1, 128), jnp.int32),
            pltpu.SMEM((n, 1, 128), jnp.int32),
            pltpu.SemaphoreType.DMA((5,)),
            pltpu.SemaphoreType.DMA((len(tables),)),
            pltpu.SemaphoreType.DMA,
            peers,
            peers,
            peers,
            peers,
            *exchange,
        ],
        compiler_params=pltpu.CompilerParams(
            collective_id=0, has_side_effects=True, vmem_limit_bytes=grant
        ),
    )(
        *tables,
        queries,
        new_keys.reshape(span // page_rows, page_rows, width),
        new_values.reshape(span // page_rows, page_rows, width),
        pool_keys,
        pool_values,
    )
    return pl.pallas_call(
        finish,
        out_shape=results,
        in_specs=[held] * 4,
        out_specs=(anywhere,) * 3,
        scratch_shapes=[
            pltpu.SMEM((1, 128), jnp.int32),
            pltpu.SemaphoreType.DMA,
            pltpu.SemaphoreType.DMA((3,)),
        ],
        compiler_params=pltpu.CompilerParams(vmem_limit_bytes=1024 * 1024),
    )(out, recv_new, pool, source)


def solution(mesh):
    rows = P(("groups", "seq"), None)
    pages = P(("groups", "seq"), None, None)
    each = P(("groups", "seq"))
    return jax.shard_map(
        shards,
        mesh=mesh,
        in_specs=(rows, rows, rows, pages, pages, each, each, rows, rows, rows, rows),
        out_specs=(rows, pages, pages),
        check_vma=False,
    )
```

```python
import functools
import math

import jax
import jax.numpy as jnp
from jax import lax
from jax.experimental import pallas as pl
from jax.experimental.pallas import tpu as pltpu
from jax.sharding import PartitionSpec as P

HEADS = 32
KV_HEADS = 8
HEAD = 128
ROWS = 128
SLOT_LANE = 64
EARLY = 5
INNER = (
    (("far", 0), ("far", 1)),
    (
        ("beside", 3),
        ("own", 0),
        ("mirror", 0),
        ("layer", 1),
        ("layer", 2),
        ("layer", 3),
        ("beside", 1),
        ("far", 2),
        ("mirror", 1),
        ("near", 1),
        ("near", 2),
        ("far", 3),
        ("beside", 2),
        ("relay", 0),
        ("relay", 1),
        ("near", 3),
    ),
    (("beside", 0), ("near", 0)),
)
OUTER = (
    (("beside", 2), ("far", 1), ("far", 2)),
    (
        ("own", 0),
        ("mirror", 0),
        ("mirror", 1),
        ("beside", 0),
        ("beside", 3),
        ("beside", 1),
        ("near", 0),
        ("near", 3),
        ("near", 1),
        ("near", 2),
        ("far", 3),
        ("layer", 1),
        ("layer", 2),
        ("layer", 3),
    ),
    (("far", 0),),
)
MESH = pl.DeviceIdType.MESH


def crosses_once(n, new_pages):
    return n == new_pages and n % 4 == 0


def kernel(
    n,
    new_pages,
    prefix_pages,
    prefix_len_hbm,
    new_len_hbm,
    page_holder_hbm,
    page_slot_hbm,
    new_holder_hbm,
    new_slot_hbm,
    q_hbm,
    k_hbm,
    v_hbm,
    pk_hbm,
    pv_hbm,
    out,
    recv_new,
    pool,
    source,
    prefix_len,
    new_len,
    page_holder,
    page_slot,
    new_holder,
    new_slot,
    q,
    kv,
    prefix,
    send_new,
    meta,
    recv_meta,
    tables,
    in_sem,
    own_sem,
    table_sem,
    meta_send_sem,
    meta_recv_sem,
    new_send_sem,
    new_recv_sem,
    *exchange,
):
    me = lax.axis_index("seq")
    mine = lax.axis_index("groups")
    halves = crosses_once(n, new_pages)
    span = q.shape[0]
    page_rows = pool.shape[2]
    slots = pool.shape[1]
    group = HEADS // KV_HEADS

    def peer(step):
        return lax.rem(me + step, n)

    barrier = pltpu.get_barrier_semaphore()

    def greet(step, carry):
        pl.semaphore_signal(barrier, inc=1, device_id=(mine, peer(step)), device_id_type=MESH)
        return carry

    lax.fori_loop(1, n, greet, 0)

    given = [
        pltpu.make_async_copy(there, here, own_sem.at[i])
        for i, (there, here) in enumerate(
            (
                (new_holder_hbm, new_holder),
                (new_slot_hbm, new_slot),
                (page_holder_hbm, page_holder),
                (page_slot_hbm, page_slot),
                (new_len_hbm, new_len),
                (prefix_len_hbm, prefix_len),
            )
        )
    ]
    for copy in given:
        copy.start()
    loads = [
        pltpu.make_async_copy(k_hbm, kv.at[0], in_sem.at[0]),
        pltpu.make_async_copy(v_hbm, kv.at[1], in_sem.at[1]),
        pltpu.make_async_copy(pk_hbm, pool.at[0], in_sem.at[2]),
        pltpu.make_async_copy(pv_hbm, pool.at[1], in_sem.at[3]),
        pltpu.make_async_copy(q_hbm, q, in_sem.at[4]),
    ]
    for load in loads:
        load.start()

    for copy in given:
        copy.wait()

    lanes = lax.broadcasted_iota(jnp.int32, meta.shape, 1)
    row = jnp.full(meta.shape, -1, jnp.int32)
    for i in range(new_pages):
        row = jnp.where(lanes == i, new_holder[0, i], row)
        row = jnp.where(lanes == SLOT_LANE + i, new_slot[0, i], row)
    for j in range(prefix_pages):
        row = jnp.where(lanes == new_pages + j, page_holder[0, j], row)
        row = jnp.where(lanes == SLOT_LANE + new_pages + j, page_slot[0, j], row)
    meta[...] = row
    recv_meta[me] = row

    live = new_len[0]
    page_pos = lax.broadcasted_iota(jnp.int32, (page_rows, kv.shape[3]), 0)

    def fill_new(target):
        page = jnp.int32(0)
        for i in range(new_pages):
            page = jnp.where(new_holder[0, i] == target, i, page)
        keep = page_pos < live - page * page_rows
        for side in range(2):
            rows = kv[side, page]
            send_new[target, side] = jnp.where(keep, rows, jnp.zeros_like(rows))

    def remote(sent, received, send_sem, recv_sem, target):
        return pltpu.make_async_remote_copy(
            src_ref=sent,
            dst_ref=received,
            send_sem=send_sem,
            recv_sem=recv_sem,
            device_id=(mine, target),
            device_id_type=MESH,
        )

    def landed(buffer, sem):
        return pltpu.make_async_copy(buffer, buffer, sem)

    def meta_copy(step):
        return remote(
            meta, recv_meta.at[me], meta_send_sem.at[step], meta_recv_sem.at[me], peer(step)
        )

    def new_to(target):
        return remote(
            send_new.at[target],
            recv_new.at[me],
            new_send_sem.at[target],
            new_recv_sem.at[me],
            target,
        )

    def arrival(step, buffer, sem):
        at = peer(step)
        return landed(buffer.at[at], sem.at[at])

    pl.semaphore_wait(barrier, n - 1)

    def each(first, last, act):
        def body(step, carry):
            act(step)
            return carry

        lax.fori_loop(first, last, body, 0)

    each(1, n, lambda step: meta_copy(step).start())
    loads[0].wait()
    loads[1].wait()

    def wanted(conversation, holder):
        slot = jnp.int32(-1)
        for j in range(prefix_pages):
            slot = jnp.where(
                tables[conversation, 0, new_pages + j] == holder,
                tables[conversation, 0, SLOT_LANE + new_pages + j],
                slot,
            )
        return slot

    def read_tables():
        each(1, n, lambda step: arrival(step, recv_meta, meta_recv_sem).wait())
        table_copy = pltpu.make_async_copy(recv_meta, tables, table_sem)
        table_copy.start()
        table_copy.wait()

    def index_incoming():
        def incoming(device, origins):
            landing = jnp.int32(-1)
            for i in range(new_pages):
                landing = jnp.where(
                    tables[device, 0, i] == me, tables[device, 0, SLOT_LANE + i], landing
                )
            return jnp.where(lanes == landing, device, origins)

        source[...] = lax.fori_loop(0, n, incoming, jnp.full(source.shape, -1, jnp.int32))

    if halves:
        (
            mirror_k,
            mirror_v,
            mirrored_k,
            mirrored_v,
            send_own,
            recv_own,
            relay_k,
            relay_v,
            recv_k,
            recv_v,
            ranks,
            mirror_send_sem,
            mirror_recv_sem,
            own_send_sem,
            own_recv_sem,
            relay_send_sem,
            relay_recv_sem,
        ) = exchange
        half, plane = n // 2, n // 4
        layer, place = me // plane, lax.rem(me, plane)
        mine_half = me // half
        base, other = mine_half * half, (1 - mine_half) * half
        inner = (layer == 1) | (layer == 2)
        here = me - base
        kept = mirror_k.shape[0]

        def in_layer(which, i):
            return which * plane + lax.rem(place + i, plane)

        layers = {
            "layer": layer,
            "beside": base // plane + 1 - lax.rem(layer, 2),
            "near": 2 - mine_half,
            "far": 3 - 3 * mine_half,
        }

        def target(which, i):
            return in_layer(layers[which], i)

        def early_fill(order):
            for which, i in order[0]:
                fill_new(target(which, i))

        def late_fill(order):
            for which, i in order[1] + order[2]:
                if which in layers:
                    fill_new(target(which, i))

        def stage(order, number):
            for which, i in order[number]:
                if which == "own":
                    each(1, half, lambda j: own_copy(j).start())
                elif which == "mirror":
                    mirror_copy(i).start()
                elif which == "relay":
                    forward(i)
                else:
                    new_to(target(which, i)).start()

        def by_layer(act):
            pl.when(inner)(functools.partial(act, INNER))
            pl.when(jnp.logical_not(inner))(functools.partial(act, OUTER))

        mirror_at = half - plane * mine_half + place
        origin = lax.rem(layer, 2)

        def mirror_copy(which):
            sent, received = ((mirror_k, mirrored_k), (mirror_v, mirrored_v))[which]
            return remote(
                sent,
                received.at[origin],
                mirror_send_sem.at[which],
                mirror_recv_sem.at[origin, which],
                mirror_at,
            )

        def half_peer(i):
            away = (i > 0) & (i <= plane)
            which = jnp.where(away, layers["beside"], layer)
            turn = place + jnp.where(away, i - 1, i)
            return which * plane + lax.rem(turn, plane) - base

        def own_copy(i):
            to = half_peer(i)
            return remote(
                send_own.at[to],
                recv_own.at[here],
                own_send_sem.at[to],
                own_recv_sem.at[here],
                base + to,
            )

        def relay_copy(i, which):
            to = half_peer(i)
            sent, received = ((relay_k, recv_k), (relay_v, recv_v))[which]
            return remote(
                sent.at[to],
                received.at[place],
                relay_send_sem.at[to, which],
                relay_recv_sem.at[place, which],
                base + to,
            )

        def forward(which):
            sent, got = ((relay_k, mirrored_k), (relay_v, mirrored_v))[which]
            received = (recv_k, recv_v)[which]
            for o in range(2):
                landed(got.at[o], mirror_recv_sem.at[o, which]).wait()

            def fill_relay(i):
                to = half_peer(i)
                for o in range(2):
                    sent[to, o] = got[o, ranks[to * 2 + o]]

            fill_relay(1)

            def relay_step(i):
                fill_relay(i)
                relay_copy(i - 1, which).start()

            each(2, half, relay_step)
            fill_relay(0)
            relay_copy(half - 1, which).start()
            received[place] = sent[here]

        by_layer(early_fill)
        by_layer(lambda order: stage(order, 0))
        by_layer(late_fill)
        fill_new(me)
        recv_new[me] = send_new[me]
        prefix[...] = jnp.zeros_like(prefix)
        loads[2].wait()
        loads[3].wait()
        read_tables()

        def pick(i, carry):
            count, picks = carry
            slot = wanted(other + i, me)
            found = slot >= 0
            picks = tuple(
                jnp.where(found & (count == k), slot, p) for k, p in enumerate(picks)
            )
            return count + jnp.where(found, 1, 0), picks

        picks = lax.fori_loop(
            0, half, pick, (jnp.int32(0), (jnp.int32(0),) * kept)
        )[1]
        for k in range(kept):
            mirror_k[k] = pool[0, picks[k]]
        for k in range(kept):
            mirror_v[k] = pool[1, picks[k]]

        def fill_own(to):
            slot = jnp.maximum(wanted(base + to, me), 0)
            for side in range(2):
                send_own[to, side] = pool[side, slot]

        each(0, half, fill_own)

        for o in range(2):
            def rank(i, count):
                ranks[i * 2 + o] = jnp.minimum(count, kept - 1)
                found = wanted(base + i, other + o * plane + place) >= 0
                return count + jnp.where(found, 1, 0)

            lax.fori_loop(0, half, rank, jnp.int32(0))

        by_layer(lambda order: stage(order, 1))
        recv_own[here] = send_own[here]
        index_incoming()
        loads[4].wait()

        each(1, half, lambda i: landed(
            recv_own.at[half_peer(i)], own_recv_sem.at[half_peer(i)]
        ).wait())
        for which in range(2):
            received = (recv_k, recv_v)[which]

            def relayed(i):
                @pl.when(jnp.logical_not(inner & (i == place)))
                def _():
                    landed(received.at[i], relay_recv_sem.at[i, which]).wait()

            each(0, plane, relayed)

        by_layer(lambda order: stage(order, 2))

        for j in range(prefix_pages):
            holder = page_holder[0, j]
            close = holder // half == mine_half
            for side in range(2):
                own = recv_own[lax.rem(holder, half), side]
                through = (recv_k, recv_v)[side][
                    lax.rem(holder, plane), lax.rem(holder // plane, 2)
                ]
                prefix[side, j * page_rows : (j + 1) * page_rows, :] = jnp.where(
                    close, own, through
                )

        def wait_pages():
            mirror_copy(0).wait_send()
            mirror_copy(1).wait_send()
            each(1, half, lambda i: own_copy(i).wait_send())

            @pl.when(inner)
            def _():
                for which in range(2):
                    each(1, half, lambda i: relay_copy(i, which).wait_send())

            each(1, n, lambda step: new_to(peer(step)).wait_send())

            def new_from(which, i):
                source = target(which, i)
                landed(recv_new.at[source], new_recv_sem.at[source]).wait()

            for which in layers:
                each(1, plane, lambda i: new_from(which, i))
            for which in ("beside", "far", "near"):
                new_from(which, 0)

    else:
        send_pre, recv_pre, pre_send_sem, pre_recv_sem = exchange

        def pre_copy(step):
            return remote(
                send_pre.at[peer(step)],
                recv_pre.at[me],
                pre_send_sem.at[step],
                pre_recv_sem.at[me],
                peer(step),
            )

        each(0, n, fill_new)
        recv_new[me] = send_new[me]
        prefix[...] = jnp.zeros_like(prefix)
        early = min(EARLY, n - 1) + 1
        each(1, early, lambda step: new_to(peer(step)).start())
        loads[2].wait()
        loads[3].wait()
        read_tables()

        def fill_pre(target):
            slot = jnp.maximum(wanted(target, me), 0)
            for side in range(2):
                send_pre[target, side] = pool[side, slot]

        fill_pre(peer(1))

        def pipelined(step):
            fill_pre(peer(step))
            pre_copy(step - 1).start()

        each(2, n, pipelined)
        fill_pre(me)
        pre_copy(n - 1).start()
        recv_pre[me] = send_pre[me]
        each(early, n, lambda step: new_to(peer(step)).start())
        index_incoming()
        loads[4].wait()

        each(1, n, lambda step: arrival(step, recv_pre, pre_recv_sem).wait())
        for j in range(prefix_pages):
            for side in range(2):
                prefix[side, j * page_rows : (j + 1) * page_rows, :] = recv_pre[
                    page_holder[0, j], side
                ]

        def wait_pages():
            each(1, n, lambda step: pre_copy(step).wait_send())
            each(1, n, lambda step: new_to(peer(step)).wait_send())
            each(1, n, lambda step: arrival(step, recv_new, new_recv_sem).wait())

    factor = math.log2(math.e) / math.sqrt(HEAD)
    nt = (((1,), (1,)), ((), ()))
    row_pos = lax.rem(lax.broadcasted_iota(jnp.int32, (group * ROWS, ROWS), 0), ROWS)
    col_pos = lax.broadcasted_iota(jnp.int32, (group * ROWS, ROWS), 1)
    prefix_pos = lax.broadcasted_iota(jnp.int32, (group * ROWS, prefix.shape[1]), 1)
    prefix_tokens = prefix_len[0]

    def head_cols(g, h):
        return pl.ds(pl.multiple_of((g * group + h) * HEAD, HEAD), HEAD)

    def attend(g):
        kv_cols = pl.ds(pl.multiple_of(g * HEAD, HEAD), HEAD)
        for block in range(span // ROWS):
            rows = slice(block * ROWS, (block + 1) * ROWS)
            keys = (block + 1) * ROWS
            query = jnp.concatenate(
                [q[rows, head_cols(g, h)] for h in range(group)], axis=0
            )
            old = lax.dot_general(
                query, prefix[0, :, kv_cols], nt, preferred_element_type=jnp.float32
            )
            fresh = lax.dot_general(
                query,
                kv[0, : keys // page_rows, :, kv_cols].reshape(keys, HEAD),
                nt,
                preferred_element_type=jnp.float32,
            )
            old = jnp.where(prefix_pos < prefix_tokens, old, -jnp.inf)
            last = jnp.where(col_pos <= row_pos, fresh[:, block * ROWS :], -jnp.inf)
            parts = [fresh[:, i * ROWS : (i + 1) * ROWS] for i in range(block)] + [last]
            top = old
            for part in parts:
                top = jnp.maximum(top, part)
            top = jnp.max(top, axis=1, keepdims=True)
            old = jnp.exp2((old - top) * factor)
            parts = [jnp.exp2((part - top) * factor) for part in parts]
            total = old
            for part in parts:
                total = total + part
            total = jnp.sum(total, axis=1, keepdims=True)
            weighted = jnp.dot(
                old.astype(jnp.bfloat16),
                prefix[1, :, kv_cols],
                preferred_element_type=jnp.float32,
            )
            weighted = weighted + jnp.dot(
                jnp.concatenate(parts, axis=1).astype(jnp.bfloat16),
                kv[1, : keys // page_rows, :, kv_cols].reshape(keys, HEAD),
                preferred_element_type=jnp.float32,
            )
            result = weighted * (1.0 / total)
            result = jnp.where(row_pos + block * ROWS < live, result, 0.0).astype(jnp.bfloat16)
            for h in range(group):
                out[rows, head_cols(g, h)] = result[h * ROWS : (h + 1) * ROWS]

    each(0, KV_HEADS, attend)

    each(1, n, lambda step: meta_copy(step).wait_send())
    wait_pages()


def finish(out, recv_new, pool, source, o_hbm, pko_hbm, pvo_hbm, origins, origin_sem, sem):
    table = pltpu.make_async_copy(source, origins, origin_sem)
    table.start()
    whole = pltpu.make_async_copy(out, o_hbm, sem.at[0])
    whole.start()
    table.wait()
    targets = (pko_hbm, pvo_hbm)

    def place(slot, carry):
        device = origins[0, slot]

        @pl.when(device >= 0)
        def _():
            for side in range(2):
                pltpu.make_async_copy(
                    recv_new.at[device, side], targets[side].at[slot], sem.at[1 + side]
                ).start()

        @pl.when(device < 0)
        def _():
            for side in range(2):
                pltpu.make_async_copy(
                    pool.at[side, slot], targets[side].at[slot], sem.at[1 + side]
                ).start()

        return carry

    lax.fori_loop(0, pool.shape[1], place, 0)
    for side in range(2):
        pltpu.make_async_copy(pool.at[side], targets[side], sem.at[1 + side]).wait()
    whole.wait()


def shards(
    queries,
    new_keys,
    new_values,
    pool_keys,
    pool_values,
    prefix_len,
    new_len,
    page_holder,
    page_slot,
    new_holder,
    new_slot,
):
    n = lax.axis_size("seq")
    slots, page_rows, width = pool_keys.shape
    span = queries.shape[0]
    new_pages = new_holder.shape[1]
    prefix_pages = page_holder.shape[1]
    padded = -(-prefix_pages * page_rows // ROWS) * ROWS
    kind = queries.dtype
    tables = (prefix_len, new_len, page_holder, page_slot, new_holder, new_slot)
    anywhere = pl.BlockSpec(memory_space=pl.ANY)
    peers = pltpu.SemaphoreType.DMA((n,))

    def pages(*count):
        return pltpu.VMEM((*count, page_rows, width), kind)

    if crosses_once(n, new_pages):
        half, plane, left = n // 2, n // 4, slots - new_pages
        exchange = [
            pages(left),
            pages(left),
            pages(2, left),
            pages(2, left),
            pages(half, 2),
            pages(half, 2),
            pages(half, 2),
            pages(half, 2),
            pages(plane, 2),
            pages(plane, 2),
            pltpu.SMEM((n,), jnp.int32),
            pltpu.SemaphoreType.DMA((2,)),
            pltpu.SemaphoreType.DMA((2, 2)),
            pltpu.SemaphoreType.DMA((half,)),
            pltpu.SemaphoreType.DMA((half,)),
            pltpu.SemaphoreType.DMA((half, 2)),
            pltpu.SemaphoreType.DMA((plane, 2)),
        ]
    else:
        exchange = [pages(n, 2), pages(n, 2), peers, peers]
    held = pl.BlockSpec(memory_space=pltpu.VMEM)
    page_bytes = 2 * page_rows * width * kind.itemsize
    kept = queries.size * kind.itemsize + (n + slots) * page_bytes + 4096
    grant = 67043328 - kept - 256 * 1024
    results = (
        jax.ShapeDtypeStruct(queries.shape, kind),
        jax.ShapeDtypeStruct(pool_keys.shape, kind),
        jax.ShapeDtypeStruct(pool_values.shape, kind),
    )
    out, recv_new, pool, source = pl.pallas_call(
        functools.partial(kernel, n, new_pages, prefix_pages),
        out_shape=(
            pltpu.VMEM(queries.shape, kind),
            pages(n, 2),
            pages(2, slots),
            pltpu.VMEM((1, 128), jnp.int32),
        ),
        in_specs=[anywhere] * 11,
        out_specs=(held,) * 4,
        scratch_shapes=[
            *[pltpu.SMEM(table.shape, table.dtype) for table in tables],
            pltpu.VMEM(queries.shape, kind),
            pltpu.VMEM((2, span // page_rows, page_rows, width), kind),
            pltpu.VMEM((2, padded, width), kind),
            pages(n, 2),
            pltpu.VMEM((1, 128), jnp.int32),
            pltpu.VMEM((n, 1, 128), jnp.int32),
            pltpu.SMEM((n, 1, 128), jnp.int32),
            pltpu.SemaphoreType.DMA((5,)),
            pltpu.SemaphoreType.DMA((len(tables),)),
            pltpu.SemaphoreType.DMA,
            peers,
            peers,
            peers,
            peers,
            *exchange,
        ],
        compiler_params=pltpu.CompilerParams(
            collective_id=0, has_side_effects=True, vmem_limit_bytes=grant
        ),
    )(
        *tables,
        queries,
        new_keys.reshape(span // page_rows, page_rows, width),
        new_values.reshape(span // page_rows, page_rows, width),
        pool_keys,
        pool_values,
    )
    return pl.pallas_call(
        finish,
        out_shape=results,
        in_specs=[held] * 4,
        out_specs=(anywhere,) * 3,
        scratch_shapes=[
            pltpu.SMEM((1, 128), jnp.int32),
            pltpu.SemaphoreType.DMA,
            pltpu.SemaphoreType.DMA((3,)),
        ],
        compiler_params=pltpu.CompilerParams(vmem_limit_bytes=1024 * 1024),
    )(out, recv_new, pool, source)


def solution(mesh):
    rows = P(("groups", "seq"), None)
    pages = P(("groups", "seq"), None, None)
    each = P(("groups", "seq"))
    return jax.shard_map(
        shards,
        mesh=mesh,
        in_specs=(rows, rows, rows, pages, pages, each, each, rows, rows, rows, rows),
        out_specs=(rows, pages, pages),
        check_vma=False,
    )
```

```python
import functools
import math

import jax
import jax.numpy as jnp
from jax import lax
from jax.experimental import pallas as pl
from jax.experimental.pallas import tpu as pltpu
from jax.sharding import PartitionSpec as P

HEADS = 32
KV_HEADS = 8
HEAD = 128
ROWS = 128
SLOT_LANE = 64
EARLY = 5
INNER = (
    (("far", 0), ("far", 1)),
    (
        ("beside", 3),
        ("own", 0),
        ("mirror", 0),
        ("layer", 1),
        ("layer", 2),
        ("layer", 3),
        ("beside", 1),
        ("far", 2),
        ("mirror", 1),
        ("near", 1),
        ("near", 2),
        ("far", 3),
        ("beside", 2),
        ("relay", 0),
        ("relay", 1),
        ("near", 3),
    ),
    (("beside", 0), ("near", 0)),
)
OUTER = (
    (("beside", 2), ("far", 1), ("far", 2)),
    (
        ("own", 0),
        ("mirror", 0),
        ("mirror", 1),
        ("beside", 0),
        ("beside", 3),
        ("beside", 1),
        ("near", 0),
        ("near", 3),
        ("near", 1),
        ("near", 2),
        ("far", 3),
        ("layer", 1),
        ("layer", 2),
        ("layer", 3),
    ),
    (("far", 0),),
)
MESH = pl.DeviceIdType.MESH


def crosses_once(n, new_pages):
    return n == new_pages and n % 4 == 0


def kernel(
    n,
    new_pages,
    prefix_pages,
    prefix_len_hbm,
    new_len_hbm,
    page_holder_hbm,
    page_slot_hbm,
    new_holder_hbm,
    new_slot_hbm,
    q_hbm,
    k_hbm,
    v_hbm,
    pk_hbm,
    pv_hbm,
    out,
    recv_new,
    pool,
    source,
    prefix_len,
    new_len,
    page_holder,
    page_slot,
    new_holder,
    new_slot,
    q,
    kv,
    prefix,
    send_new,
    meta,
    recv_meta,
    tables,
    in_sem,
    own_sem,
    table_sem,
    meta_send_sem,
    meta_recv_sem,
    new_send_sem,
    new_recv_sem,
    *exchange,
):
    me = lax.axis_index("seq")
    mine = lax.axis_index("groups")
    halves = crosses_once(n, new_pages)
    span = q.shape[0]
    page_rows = pool.shape[2]
    slots = pool.shape[1]
    group = HEADS // KV_HEADS

    def peer(step):
        return lax.rem(me + step, n)

    barrier = pltpu.get_barrier_semaphore()

    def greet(step, carry):
        pl.semaphore_signal(barrier, inc=1, device_id=(mine, peer(step)), device_id_type=MESH)
        return carry

    lax.fori_loop(1, n, greet, 0, unroll=halves)

    given = [
        pltpu.make_async_copy(there, here, own_sem.at[i])
        for i, (there, here) in enumerate(
            (
                (new_holder_hbm, new_holder),
                (new_slot_hbm, new_slot),
                (page_holder_hbm, page_holder),
                (page_slot_hbm, page_slot),
                (new_len_hbm, new_len),
                (prefix_len_hbm, prefix_len),
            )
        )
    ]
    for copy in given:
        copy.start()
    loads = [
        pltpu.make_async_copy(k_hbm, kv.at[0], in_sem.at[0]),
        pltpu.make_async_copy(v_hbm, kv.at[1], in_sem.at[1]),
        pltpu.make_async_copy(pk_hbm, pool.at[0], in_sem.at[2]),
        pltpu.make_async_copy(pv_hbm, pool.at[1], in_sem.at[3]),
        pltpu.make_async_copy(q_hbm, q, in_sem.at[4]),
    ]
    for load in loads:
        load.start()

    for copy in given:
        copy.wait()

    lanes = lax.broadcasted_iota(jnp.int32, meta.shape, 1)
    row = jnp.full(meta.shape, -1, jnp.int32)
    for i in range(new_pages):
        row = jnp.where(lanes == i, new_holder[0, i], row)
        row = jnp.where(lanes == SLOT_LANE + i, new_slot[0, i], row)
    for j in range(prefix_pages):
        row = jnp.where(lanes == new_pages + j, page_holder[0, j], row)
        row = jnp.where(lanes == SLOT_LANE + new_pages + j, page_slot[0, j], row)
    meta[...] = row
    recv_meta[me] = row

    live = new_len[0]
    page_pos = lax.broadcasted_iota(jnp.int32, (page_rows, kv.shape[3]), 0)

    def fill_new(target):
        page = jnp.int32(0)
        for i in range(new_pages):
            page = jnp.where(new_holder[0, i] == target, i, page)
        keep = page_pos < live - page * page_rows
        for side in range(2):
            rows = kv[side, page]
            send_new[target, side] = jnp.where(keep, rows, jnp.zeros_like(rows))

    def remote(sent, received, send_sem, recv_sem, target):
        return pltpu.make_async_remote_copy(
            src_ref=sent,
            dst_ref=received,
            send_sem=send_sem,
            recv_sem=recv_sem,
            device_id=(mine, target),
            device_id_type=MESH,
        )

    def landed(buffer, sem):
        return pltpu.make_async_copy(buffer, buffer, sem)

    def meta_copy(step):
        return remote(
            meta, recv_meta.at[me], meta_send_sem.at[step], meta_recv_sem.at[me], peer(step)
        )

    def new_to(target):
        return remote(
            send_new.at[target],
            recv_new.at[me],
            new_send_sem.at[target],
            new_recv_sem.at[me],
            target,
        )

    def arrival(step, buffer, sem):
        at = peer(step)
        return landed(buffer.at[at], sem.at[at])

    pl.semaphore_wait(barrier, n - 1)

    def each(first, last, act):
        def body(step, carry):
            act(step)
            return carry

        lax.fori_loop(first, last, body, 0)

    if halves:
        for step in range(1, n):
            meta_copy(step).start()
    else:
        each(1, n, lambda step: meta_copy(step).start())
    loads[0].wait()
    loads[1].wait()

    def wanted(conversation, holder):
        slot = jnp.int32(-1)
        for j in range(prefix_pages):
            slot = jnp.where(
                tables[conversation, 0, new_pages + j] == holder,
                tables[conversation, 0, SLOT_LANE + new_pages + j],
                slot,
            )
        return slot

    def read_tables():
        each(1, n, lambda step: arrival(step, recv_meta, meta_recv_sem).wait())
        table_copy = pltpu.make_async_copy(recv_meta, tables, table_sem)
        table_copy.start()
        table_copy.wait()

    def index_incoming():
        def incoming(device, origins):
            landing = jnp.int32(-1)
            for i in range(new_pages):
                landing = jnp.where(
                    tables[device, 0, i] == me, tables[device, 0, SLOT_LANE + i], landing
                )
            return jnp.where(lanes == landing, device, origins)

        source[...] = lax.fori_loop(0, n, incoming, jnp.full(source.shape, -1, jnp.int32))

    if halves:
        (
            mirror_k,
            mirror_v,
            mirrored_k,
            mirrored_v,
            send_own,
            recv_own,
            relay_k,
            relay_v,
            recv_k,
            recv_v,
            ranks,
            mirror_send_sem,
            mirror_recv_sem,
            own_send_sem,
            own_recv_sem,
            relay_send_sem,
            relay_recv_sem,
        ) = exchange
        half, plane = n // 2, n // 4
        layer, place = me // plane, lax.rem(me, plane)
        mine_half = me // half
        base, other = mine_half * half, (1 - mine_half) * half
        inner = (layer == 1) | (layer == 2)
        here = me - base
        kept = mirror_k.shape[0]

        def in_layer(which, i):
            return which * plane + lax.rem(place + i, plane)

        layers = {
            "layer": layer,
            "beside": base // plane + 1 - lax.rem(layer, 2),
            "near": 2 - mine_half,
            "far": 3 - 3 * mine_half,
        }

        def target(which, i):
            return in_layer(layers[which], i)

        def early_fill(order):
            for which, i in order[0]:
                fill_new(target(which, i))

        def late_fill(order):
            for which, i in order[1] + order[2]:
                if which in layers:
                    fill_new(target(which, i))

        def stage(order, number):
            for which, i in order[number]:
                if which == "own":
                    each(1, half, lambda j: own_copy(j).start())
                elif which == "mirror":
                    mirror_copy(i).start()
                elif which == "relay":
                    forward(i)
                else:
                    new_to(target(which, i)).start()

        def by_layer(act):
            pl.when(inner)(functools.partial(act, INNER))
            pl.when(jnp.logical_not(inner))(functools.partial(act, OUTER))

        mirror_at = half - plane * mine_half + place
        origin = lax.rem(layer, 2)

        def mirror_copy(which):
            sent, received = ((mirror_k, mirrored_k), (mirror_v, mirrored_v))[which]
            return remote(
                sent,
                received.at[origin],
                mirror_send_sem.at[which],
                mirror_recv_sem.at[origin, which],
                mirror_at,
            )

        def half_peer(i):
            away = (i > 0) & (i <= plane)
            which = jnp.where(away, layers["beside"], layer)
            turn = place + jnp.where(away, i - 1, i)
            return which * plane + lax.rem(turn, plane) - base

        def own_copy(i):
            to = half_peer(i)
            return remote(
                send_own.at[to],
                recv_own.at[here],
                own_send_sem.at[to],
                own_recv_sem.at[here],
                base + to,
            )

        def relay_copy(i, which):
            to = half_peer(i)
            sent, received = ((relay_k, recv_k), (relay_v, recv_v))[which]
            return remote(
                sent.at[to],
                received.at[place],
                relay_send_sem.at[to, which],
                relay_recv_sem.at[place, which],
                base + to,
            )

        def forward(which):
            sent, got = ((relay_k, mirrored_k), (relay_v, mirrored_v))[which]
            received = (recv_k, recv_v)[which]
            for o in range(2):
                landed(got.at[o], mirror_recv_sem.at[o, which]).wait()

            def fill_relay(i):
                to = half_peer(i)
                for o in range(2):
                    sent[to, o] = got[o, ranks[to * 2 + o]]

            fill_relay(1)

            def relay_step(i):
                fill_relay(i)
                relay_copy(i - 1, which).start()

            each(2, half, relay_step)
            fill_relay(0)
            relay_copy(half - 1, which).start()
            received[place] = sent[here]

        by_layer(early_fill)
        by_layer(lambda order: stage(order, 0))
        by_layer(late_fill)
        fill_new(me)
        recv_new[me] = send_new[me]
        prefix[...] = jnp.zeros_like(prefix)
        loads[2].wait()
        loads[3].wait()
        read_tables()

        def pick(i, carry):
            count, picks = carry
            slot = wanted(other + i, me)
            found = slot >= 0
            picks = tuple(
                jnp.where(found & (count == k), slot, p) for k, p in enumerate(picks)
            )
            return count + jnp.where(found, 1, 0), picks

        picks = lax.fori_loop(
            0, half, pick, (jnp.int32(0), (jnp.int32(0),) * kept)
        )[1]
        for k in range(kept):
            mirror_k[k] = pool[0, picks[k]]
        for k in range(kept):
            mirror_v[k] = pool[1, picks[k]]

        def fill_own(to):
            slot = jnp.maximum(wanted(base + to, me), 0)
            for side in range(2):
                send_own[to, side] = pool[side, slot]

        each(0, half, fill_own)

        for o in range(2):
            def rank(i, count):
                ranks[i * 2 + o] = jnp.minimum(count, kept - 1)
                found = wanted(base + i, other + o * plane + place) >= 0
                return count + jnp.where(found, 1, 0)

            lax.fori_loop(0, half, rank, jnp.int32(0))

        by_layer(lambda order: stage(order, 1))
        recv_own[here] = send_own[here]
        index_incoming()
        loads[4].wait()

        each(1, half, lambda i: landed(
            recv_own.at[half_peer(i)], own_recv_sem.at[half_peer(i)]
        ).wait())
        for which in range(2):
            received = (recv_k, recv_v)[which]

            def relayed(i):
                @pl.when(jnp.logical_not(inner & (i == place)))
                def _():
                    landed(received.at[i], relay_recv_sem.at[i, which]).wait()

            each(0, plane, relayed)

        by_layer(lambda order: stage(order, 2))

        for j in range(prefix_pages):
            holder = page_holder[0, j]
            close = holder // half == mine_half
            for side in range(2):
                own = recv_own[lax.rem(holder, half), side]
                through = (recv_k, recv_v)[side][
                    lax.rem(holder, plane), lax.rem(holder // plane, 2)
                ]
                prefix[side, j * page_rows : (j + 1) * page_rows, :] = jnp.where(
                    close, own, through
                )

        def wait_pages():
            mirror_copy(0).wait_send()
            mirror_copy(1).wait_send()
            each(1, half, lambda i: own_copy(i).wait_send())

            @pl.when(inner)
            def _():
                for which in range(2):
                    each(1, half, lambda i: relay_copy(i, which).wait_send())

            each(1, n, lambda step: new_to(peer(step)).wait_send())

            def new_from(which, i):
                source = target(which, i)
                landed(recv_new.at[source], new_recv_sem.at[source]).wait()

            for which in layers:
                each(1, plane, lambda i: new_from(which, i))
            for which in ("beside", "far", "near"):
                new_from(which, 0)

    else:
        send_pre, recv_pre, pre_send_sem, pre_recv_sem = exchange

        def pre_copy(step):
            return remote(
                send_pre.at[peer(step)],
                recv_pre.at[me],
                pre_send_sem.at[step],
                pre_recv_sem.at[me],
                peer(step),
            )

        each(0, n, fill_new)
        recv_new[me] = send_new[me]
        prefix[...] = jnp.zeros_like(prefix)
        early = min(EARLY, n - 1) + 1
        each(1, early, lambda step: new_to(peer(step)).start())
        loads[2].wait()
        loads[3].wait()
        read_tables()

        def fill_pre(target):
            slot = jnp.maximum(wanted(target, me), 0)
            for side in range(2):
                send_pre[target, side] = pool[side, slot]

        fill_pre(peer(1))

        def pipelined(step):
            fill_pre(peer(step))
            pre_copy(step - 1).start()

        each(2, n, pipelined)
        fill_pre(me)
        pre_copy(n - 1).start()
        recv_pre[me] = send_pre[me]
        each(early, n, lambda step: new_to(peer(step)).start())
        index_incoming()
        loads[4].wait()

        each(1, n, lambda step: arrival(step, recv_pre, pre_recv_sem).wait())
        for j in range(prefix_pages):
            for side in range(2):
                prefix[side, j * page_rows : (j + 1) * page_rows, :] = recv_pre[
                    page_holder[0, j], side
                ]

        def wait_pages():
            each(1, n, lambda step: pre_copy(step).wait_send())
            each(1, n, lambda step: new_to(peer(step)).wait_send())
            each(1, n, lambda step: arrival(step, recv_new, new_recv_sem).wait())

    factor = math.log2(math.e) / math.sqrt(HEAD)
    nt = (((1,), (1,)), ((), ()))
    row_pos = lax.rem(lax.broadcasted_iota(jnp.int32, (group * ROWS, ROWS), 0), ROWS)
    col_pos = lax.broadcasted_iota(jnp.int32, (group * ROWS, ROWS), 1)
    prefix_pos = lax.broadcasted_iota(jnp.int32, (group * ROWS, prefix.shape[1]), 1)
    prefix_tokens = prefix_len[0]

    def head_cols(g, h):
        return pl.ds(pl.multiple_of((g * group + h) * HEAD, HEAD), HEAD)

    def attend(g):
        kv_cols = pl.ds(pl.multiple_of(g * HEAD, HEAD), HEAD)
        for block in range(span // ROWS):
            rows = slice(block * ROWS, (block + 1) * ROWS)
            keys = (block + 1) * ROWS
            query = jnp.concatenate(
                [q[rows, head_cols(g, h)] for h in range(group)], axis=0
            )
            old = lax.dot_general(
                query, prefix[0, :, kv_cols], nt, preferred_element_type=jnp.float32
            )
            fresh = lax.dot_general(
                query,
                kv[0, : keys // page_rows, :, kv_cols].reshape(keys, HEAD),
                nt,
                preferred_element_type=jnp.float32,
            )
            old = jnp.where(prefix_pos < prefix_tokens, old, -jnp.inf)
            last = jnp.where(col_pos <= row_pos, fresh[:, block * ROWS :], -jnp.inf)
            parts = [fresh[:, i * ROWS : (i + 1) * ROWS] for i in range(block)] + [last]
            top = old
            for part in parts:
                top = jnp.maximum(top, part)
            top = jnp.max(top, axis=1, keepdims=True)
            old = jnp.exp2((old - top) * factor)
            parts = [jnp.exp2((part - top) * factor) for part in parts]
            total = old
            for part in parts:
                total = total + part
            total = jnp.sum(total, axis=1, keepdims=True)
            weighted = jnp.dot(
                old.astype(jnp.bfloat16),
                prefix[1, :, kv_cols],
                preferred_element_type=jnp.float32,
            )
            weighted = weighted + jnp.dot(
                jnp.concatenate(parts, axis=1).astype(jnp.bfloat16),
                kv[1, : keys // page_rows, :, kv_cols].reshape(keys, HEAD),
                preferred_element_type=jnp.float32,
            )
            result = weighted * (1.0 / total)
            result = jnp.where(row_pos + block * ROWS < live, result, 0.0).astype(jnp.bfloat16)
            for h in range(group):
                out[rows, head_cols(g, h)] = result[h * ROWS : (h + 1) * ROWS]

    each(0, KV_HEADS, attend)

    each(1, n, lambda step: meta_copy(step).wait_send())
    wait_pages()


def finish(out, recv_new, pool, source, o_hbm, pko_hbm, pvo_hbm, origins, origin_sem, sem):
    table = pltpu.make_async_copy(source, origins, origin_sem)
    table.start()
    whole = pltpu.make_async_copy(out, o_hbm, sem.at[0])
    whole.start()
    table.wait()
    targets = (pko_hbm, pvo_hbm)

    def place(slot, carry):
        device = origins[0, slot]

        @pl.when(device >= 0)
        def _():
            for side in range(2):
                pltpu.make_async_copy(
                    recv_new.at[device, side], targets[side].at[slot], sem.at[1 + side]
                ).start()

        @pl.when(device < 0)
        def _():
            for side in range(2):
                pltpu.make_async_copy(
                    pool.at[side, slot], targets[side].at[slot], sem.at[1 + side]
                ).start()

        return carry

    lax.fori_loop(0, pool.shape[1], place, 0)
    for side in range(2):
        pltpu.make_async_copy(pool.at[side], targets[side], sem.at[1 + side]).wait()
    whole.wait()


def shards(
    queries,
    new_keys,
    new_values,
    pool_keys,
    pool_values,
    prefix_len,
    new_len,
    page_holder,
    page_slot,
    new_holder,
    new_slot,
):
    n = lax.axis_size("seq")
    slots, page_rows, width = pool_keys.shape
    span = queries.shape[0]
    new_pages = new_holder.shape[1]
    prefix_pages = page_holder.shape[1]
    padded = -(-prefix_pages * page_rows // ROWS) * ROWS
    kind = queries.dtype
    tables = (prefix_len, new_len, page_holder, page_slot, new_holder, new_slot)
    anywhere = pl.BlockSpec(memory_space=pl.ANY)
    peers = pltpu.SemaphoreType.DMA((n,))

    def pages(*count):
        return pltpu.VMEM((*count, page_rows, width), kind)

    if crosses_once(n, new_pages):
        half, plane, left = n // 2, n // 4, slots - new_pages
        exchange = [
            pages(left),
            pages(left),
            pages(2, left),
            pages(2, left),
            pages(half, 2),
            pages(half, 2),
            pages(half, 2),
            pages(half, 2),
            pages(plane, 2),
            pages(plane, 2),
            pltpu.SMEM((n,), jnp.int32),
            pltpu.SemaphoreType.DMA((2,)),
            pltpu.SemaphoreType.DMA((2, 2)),
            pltpu.SemaphoreType.DMA((half,)),
            pltpu.SemaphoreType.DMA((half,)),
            pltpu.SemaphoreType.DMA((half, 2)),
            pltpu.SemaphoreType.DMA((plane, 2)),
        ]
    else:
        exchange = [pages(n, 2), pages(n, 2), peers, peers]
    held = pl.BlockSpec(memory_space=pltpu.VMEM)
    page_bytes = 2 * page_rows * width * kind.itemsize
    kept = queries.size * kind.itemsize + (n + slots) * page_bytes + 4096
    grant = 67043328 - kept - 256 * 1024
    results = (
        jax.ShapeDtypeStruct(queries.shape, kind),
        jax.ShapeDtypeStruct(pool_keys.shape, kind),
        jax.ShapeDtypeStruct(pool_values.shape, kind),
    )
    out, recv_new, pool, source = pl.pallas_call(
        functools.partial(kernel, n, new_pages, prefix_pages),
        out_shape=(
            pltpu.VMEM(queries.shape, kind),
            pages(n, 2),
            pages(2, slots),
            pltpu.VMEM((1, 128), jnp.int32),
        ),
        in_specs=[anywhere] * 11,
        out_specs=(held,) * 4,
        scratch_shapes=[
            *[pltpu.SMEM(table.shape, table.dtype) for table in tables],
            pltpu.VMEM(queries.shape, kind),
            pltpu.VMEM((2, span // page_rows, page_rows, width), kind),
            pltpu.VMEM((2, padded, width), kind),
            pages(n, 2),
            pltpu.VMEM((1, 128), jnp.int32),
            pltpu.VMEM((n, 1, 128), jnp.int32),
            pltpu.SMEM((n, 1, 128), jnp.int32),
            pltpu.SemaphoreType.DMA((5,)),
            pltpu.SemaphoreType.DMA((len(tables),)),
            pltpu.SemaphoreType.DMA,
            peers,
            peers,
            peers,
            peers,
            *exchange,
        ],
        compiler_params=pltpu.CompilerParams(
            collective_id=0, has_side_effects=True, vmem_limit_bytes=grant
        ),
    )(
        *tables,
        queries,
        new_keys.reshape(span // page_rows, page_rows, width),
        new_values.reshape(span // page_rows, page_rows, width),
        pool_keys,
        pool_values,
    )
    return pl.pallas_call(
        finish,
        out_shape=results,
        in_specs=[held] * 4,
        out_specs=(anywhere,) * 3,
        scratch_shapes=[
            pltpu.SMEM((1, 128), jnp.int32),
            pltpu.SemaphoreType.DMA,
            pltpu.SemaphoreType.DMA((3,)),
        ],
        compiler_params=pltpu.CompilerParams(vmem_limit_bytes=1024 * 1024),
    )(out, recv_new, pool, source)


def solution(mesh):
    rows = P(("groups", "seq"), None)
    pages = P(("groups", "seq"), None, None)
    each = P(("groups", "seq"))
    return jax.shard_map(
        shards,
        mesh=mesh,
        in_specs=(rows, rows, rows, pages, pages, each, each, rows, rows, rows, rows),
        out_specs=(rows, pages, pages),
        check_vma=False,
    )
```
